32 devices in a mesh: data: 8 (over z, y), expert: 4 (over x, core).
Axes of the slice: x: 2, y: 2, z: 4, core: 2. Of those that a mesh axis runs over, the one named last changes fastest.
Arguments:
- dy: bfloat16 [32768, 768], P(('data', 'expert'))
- gates: float32 [32768, 1], P(('data', 'expert'))
- topk_idx: int32 [32768, 1], P(('data', 'expert'))
- slot: int32 [32768, 1], P(('data', 'expert'))
- yd: bfloat16 [32768, 1, 768], P(('data', 'expert'))
- xd: bfloat16 [64, 640, 768], P(('data', 'expert'))
- h1: bfloat16 [64, 640, 3072], P(('data', 'expert'))
- h3: bfloat16 [64, 640, 3072], P(('data', 'expert'))
- w1: bfloat16 [8, 768, 3072], P('expert')
- w3: bfloat16 [8, 768, 3072], P('expert')
- w2: bfloat16 [8, 3072, 768], P('expert')
Outputs:
- output 1: bfloat16 [32768, 768], P(('data', 'expert'))
- output 2: float32 [32768, 1], P(('data', 'expert'))
- output 3: float32 [8, 768, 3072], P('expert', None, 'data')
- output 4: float32 [8, 768, 3072], P('expert', None, 'data')
- output 5: float32 [8, 3072, 768], P('expert', 'data')
All inputs are finite; a program needn't handle non-finite values.
Results may differ from the reference program's by a relative error of at most 0.00861423.
Values are sent between devices in bfloat16 or wider.
A program may use at most 1 GiB of HBM per device.

```python
import jax
import jax.numpy as jnp
from jax import lax

NDATA = 8
NEXP = 4
TOKENS = 1024
EXPERTS = 8
TOPK = 1
DMODEL = 768
FF = 3072
CAP = 160

NTOK = NDATA * NEXP * TOKENS
NDEV = NDATA * NEXP
NBUF = NEXP * CAP


def _routes(topk_idx, slot):
    dev = jnp.arange(NTOK, dtype=jnp.int32) // TOKENS
    row = (dev // NEXP)[:, None] * EXPERTS + topk_idx
    col = jnp.where(slot >= 0, (dev % NEXP)[:, None] * CAP + slot, NBUF)
    return row, col


def _slots(topk_idx):
    def one(idx):
        oh = (idx.reshape(-1)[:, None] == jnp.arange(EXPERTS, dtype=jnp.int32)[None, :]).astype(jnp.int32)
        rank = jnp.sum((jnp.cumsum(oh, axis=0) - oh) * oh, axis=1)
        return jnp.where(rank < CAP, rank, -1).reshape(TOKENS, TOPK)
    return lax.map(one, topk_idx.reshape(NDEV, TOKENS, TOPK)).reshape(NTOK, TOPK).astype(jnp.int32)


def _forward(x, topk_idx, slot, w1, w3, w2):
    row, col = _routes(topk_idx, slot)
    xin = jnp.broadcast_to(x[:, None, :], (NTOK, TOPK, DMODEL))
    xd = jnp.zeros((NDATA * EXPERTS, NBUF, DMODEL), jnp.bfloat16).at[row, col].set(xin, mode='drop')
    x4 = xd.reshape(NDATA, EXPERTS, NBUF, DMODEL)

    def one(e):
        xs = x4[:, e].reshape(NDATA * NBUF, DMODEL)
        h1 = jnp.dot(xs, w1[e], preferred_element_type=jnp.float32).astype(jnp.bfloat16)
        h3 = jnp.dot(xs, w3[e], preferred_element_type=jnp.float32).astype(jnp.bfloat16)
        h1f = h1.astype(jnp.float32)
        a = (h1f * jax.nn.sigmoid(h1f) * h3.astype(jnp.float32)).astype(jnp.bfloat16)
        y = jnp.dot(a, w2[e], preferred_element_type=jnp.float32).astype(jnp.bfloat16)
        return h1.reshape(NDATA, NBUF, FF), h3.reshape(NDATA, NBUF, FF), y.reshape(NDATA, NBUF, DMODEL)

    h1, h3, y = lax.map(one, jnp.arange(EXPERTS))
    flat = lambda a: jnp.swapaxes(a, 0, 1).reshape(NDATA * EXPERTS, NBUF, a.shape[-1])
    h1, h3, y = flat(h1), flat(h3), flat(y)
    yd = jnp.where((slot >= 0)[:, :, None], y[row, jnp.minimum(col, NBUF - 1)], jnp.zeros((), jnp.bfloat16))
    return xd, h1, h3, yd


def _draw_routes(bias_key, pick_key):
    level_parts = jax.random.randint(bias_key, (4, NDEV, EXPERTS), 0, 4, jnp.int32)
    levels = jnp.sum(level_parts, axis=0)
    weights = jnp.left_shift(jnp.ones_like(levels), levels)
    tok_dev = jnp.arange(NTOK, dtype=jnp.int32) // TOKENS
    row_weights = weights[tok_dev]
    pick_keys = jax.random.split(pick_key, TOPK)
    columns = jnp.arange(EXPERTS, dtype=jnp.int32)[None, :]
    chosen = []
    for choice_idx in range(TOPK):
        bounds = jnp.cumsum(row_weights, axis=1)
        draw_value = jax.random.randint(pick_keys[choice_idx], (NTOK,), 0, bounds[:, -1], jnp.int32)
        pick_now = jnp.sum(bounds <= draw_value[:, None], axis=1, dtype=jnp.int32)
        chosen.append(pick_now)
        row_weights = jnp.where(columns == pick_now[:, None], 0, row_weights)
    return jnp.stack(chosen, axis=1).astype(jnp.int32)


def setup_inputs(seed: int = 0) -> dict:
    ks = jax.random.split(jax.random.PRNGKey(seed), 8)
    x = jax.random.normal(ks[0], (NTOK, DMODEL), jnp.float32).astype(jnp.bfloat16)
    w1 = (jax.random.normal(ks[1], (EXPERTS, DMODEL, FF), jnp.float32) * DMODEL ** -0.5).astype(jnp.bfloat16)
    w3 = (jax.random.normal(ks[2], (EXPERTS, DMODEL, FF), jnp.float32) * DMODEL ** -0.5).astype(jnp.bfloat16)
    w2 = (jax.random.normal(ks[3], (EXPERTS, FF, DMODEL), jnp.float32) * FF ** -0.5).astype(jnp.bfloat16)
    rk = jax.random.split(jax.random.fold_in(ks[4], 7), 2)
    topk_idx = _draw_routes(rk[0], rk[1])
    slot = _slots(topk_idx)
    gates = jax.random.uniform(ks[5], (NTOK, TOPK), jnp.float32, 0.2, 1.0)
    dy = jax.random.normal(ks[6], (NTOK, DMODEL), jnp.float32).astype(jnp.bfloat16)
    xd, h1, h3, yd = _forward(x, topk_idx, slot, w1, w3, w2)
    return dict(dy=dy, gates=gates, topk_idx=topk_idx, slot=slot, yd=yd, xd=xd, h1=h1, h3=h3, w1=w1, w3=w3, w2=w2)


def reference(dy, gates, topk_idx, slot, yd, xd, h1, h3, w1, w3, w2):
    row, col = _routes(topk_idx, slot)
    dyf = dy.astype(jnp.float32)
    dg = jnp.sum(yd.astype(jnp.float32) * dyf[:, None, :], axis=-1)
    v = (gates[:, :, None] * dyf[:, None, :]).astype(jnp.bfloat16)
    dyd = jnp.zeros((NDATA * EXPERTS, NBUF, DMODEL), jnp.bfloat16).at[row, col].set(v, mode='drop')
    grp = lambda a: a.reshape(NDATA, EXPERTS, NBUF, a.shape[-1])
    g4, x4, a14, a34 = grp(dyd), grp(xd), grp(h1), grp(h3)

    def one(e):
        g = g4[:, e].reshape(NDATA * NBUF, DMODEL)
        x = x4[:, e].reshape(NDATA * NBUF, DMODEL)
        h1f = a14[:, e].reshape(NDATA * NBUF, FF).astype(jnp.float32)
        h3f = a34[:, e].reshape(NDATA * NBUF, FF).astype(jnp.float32)
        s = jax.nn.sigmoid(h1f)
        silu = h1f * s
        a = (silu * h3f).astype(jnp.bfloat16)
        da = jnp.dot(g, w2[e].T, preferred_element_type=jnp.float32).astype(jnp.bfloat16).astype(jnp.float32)
        dh1 = (da * h3f * s * (1.0 + h1f * (1.0 - s))).astype(jnp.bfloat16)
        dh3 = (da * silu).astype(jnp.bfloat16)
        dw2 = jnp.dot(a.T, g, preferred_element_type=jnp.float32)
        dw1 = jnp.dot(x.T, dh1, preferred_element_type=jnp.float32)
        dw3 = jnp.dot(x.T, dh3, preferred_element_type=jnp.float32)
        dxd = (jnp.dot(dh1, w1[e].T, preferred_element_type=jnp.float32)
               + jnp.dot(dh3, w3[e].T, preferred_element_type=jnp.float32)).astype(jnp.bfloat16)
        return dw1, dw3, dw2, dxd.reshape(NDATA, NBUF, DMODEL)

    dw1, dw3, dw2, dxd = lax.map(one, jnp.arange(EXPERTS))
    dxd = jnp.swapaxes(dxd, 0, 1).reshape(NDATA * EXPERTS, NBUF, DMODEL)
    back = dxd[row, jnp.minimum(col, NBUF - 1)].astype(jnp.float32)
    dx = jnp.sum(jnp.where((slot >= 0)[:, :, None], back, 0.0), axis=1).astype(jnp.bfloat16)
    return dx, dg, dw1, dw3, dw2
```

```python
import functools

import jax
import jax.numpy as jnp
from jax import lax
from jax.experimental import pallas as pl
from jax.experimental.pallas import tpu as pltpu
from jax.sharding import PartitionSpec as P

F32 = jnp.float32
BF16 = jnp.bfloat16


RING = (0, 2, 4, 6, 7, 5, 3, 1)
RIGHT = [(RING[i], RING[(i + 1) % 8]) for i in range(8)]
LEFT = [(RING[(i + 1) % 8], RING[i]) for i in range(8)]
TILE = 256


def _dw_kernel(e, first, idx_ref, xa, xb, ya, yb, w1, w3, w2, *rest):
    o1, o3, o2 = rest[-13:-10]
    x, y, w13, w2s, dh, a, acc13, acc2, sem, osem = rest[-10:]
    rows = xa.shape[0]
    fs = w2s.shape[0]
    f0 = pl.multiple_of(idx_ref[0] * fs, 128)
    cps = [
        pltpu.make_async_copy(w1.at[e, :, pl.ds(f0, fs)], w13.at[:, pl.ds(0, fs)], sem.at[0]),
        pltpu.make_async_copy(w3.at[e, :, pl.ds(f0, fs)], w13.at[:, pl.ds(fs, fs)], sem.at[1]),
        pltpu.make_async_copy(xa, x.at[pl.ds(0, rows)], sem.at[2]),
        pltpu.make_async_copy(xb, x.at[pl.ds(rows, rows)], sem.at[3]),
        pltpu.make_async_copy(w2.at[e, pl.ds(f0, fs), :], w2s, sem.at[4]),
        pltpu.make_async_copy(ya, y.at[pl.ds(0, rows)], sem.at[5]),
        pltpu.make_async_copy(yb, y.at[pl.ds(rows, rows)], sem.at[6]),
    ]
    if not first:
        cps += [
            pltpu.make_async_copy(o1.at[e], acc13.at[:, pl.ds(0, fs)], sem.at[7]),
            pltpu.make_async_copy(o3.at[e], acc13.at[:, pl.ds(fs, fs)], sem.at[8]),
            pltpu.make_async_copy(o2.at[e], acc2, sem.at[9]),
        ]
    for c in cps:
        c.start()
    for c in cps[:7]:
        c.wait()

    def rows_body(i, _):
        r = pl.ds(pl.multiple_of(i * TILE, TILE), TILE)
        h = jnp.dot(x[r, :], w13[...], preferred_element_type=F32).astype(BF16).astype(F32)
        da = lax.dot_general(y[r, :], w2s[...], (((1,), (1,)), ((), ())),
                             preferred_element_type=F32).astype(BF16).astype(F32)
        h1, h3 = h[:, :fs], h[:, fs:]
        s = jax.nn.sigmoid(h1)
        silu = h1 * s
        a[r, :] = (silu * h3).astype(BF16)
        dh[r, :fs] = (da * h3 * s * (1.0 + h1 * (1.0 - s))).astype(BF16)
        dh[r, fs:] = (da * silu).astype(BF16)
        return 0

    lax.fori_loop(0, 2 * rows // TILE, rows_body, 0)
    for c in cps[7:]:
        c.wait()

    def acc(ref, m, val):
        if first:
            ref[m, :] = val
        else:
            ref[m, :] += val

    def d2_body(i, _):
        m = pl.ds(pl.multiple_of(i * 128, 128), 128)
        acc(acc2, m, lax.dot_general(a[:, m], y[...], (((0,), (0,)), ((), ())), preferred_element_type=F32))
        return 0

    lax.fori_loop(0, fs // 128, d2_body, 0)
    c2 = pltpu.make_async_copy(acc2, o2.at[e], osem.at[0])
    c2.start()

    def d13_body(i, _):
        m = pl.ds(pl.multiple_of(i * TILE, TILE), TILE)
        acc(acc13, m, lax.dot_general(x[:, m], dh[...], (((0,), (0,)), ((), ())), preferred_element_type=F32))
        return 0

    lax.fori_loop(0, x.shape[1] // TILE, d13_body, 0)
    c1 = pltpu.make_async_copy(acc13.at[:, pl.ds(0, fs)], o1.at[e], osem.at[1])
    c3 = pltpu.make_async_copy(acc13.at[:, pl.ds(fs, fs)], o3.at[e], osem.at[2])
    c1.start()
    c3.start()
    c2.wait()
    c1.wait()
    c3.wait()


def _dw_call(e, idx, xs, ys, w1, w3, w2, acc):
    el, d, f = w1.shape
    rows = xs[0].shape[0]
    fs = f // 8
    first = acc is None or acc[0] is None
    anyspec = pl.BlockSpec(memory_space=pl.ANY)
    outs = [jax.ShapeDtypeStruct((el, d, fs), F32), jax.ShapeDtypeStruct((el, d, fs), F32),
            jax.ShapeDtypeStruct((el, fs, d), F32)]
    args = [idx, xs[0], xs[1], ys[0], ys[1], w1, w3, w2]
    alias = {}
    prev = acc[1] if acc is not None else None
    if prev is not None:
        alias = {len(args) + i: i for i in range(3)}
        args += list(prev)
    return pl.pallas_call(
        functools.partial(_dw_kernel, e, first),
        out_shape=outs,
        in_specs=[pl.BlockSpec(memory_space=pltpu.SMEM)] + [anyspec] * (len(args) - 1),
        out_specs=[anyspec] * 3,
        scratch_shapes=[
            pltpu.VMEM((2 * rows, d), BF16),
            pltpu.VMEM((2 * rows, d), BF16),
            pltpu.VMEM((d, 2 * fs), BF16),
            pltpu.VMEM((fs, d), BF16),
            pltpu.VMEM((2 * rows, 2 * fs), BF16),
            pltpu.VMEM((2 * rows, fs), BF16),
            pltpu.VMEM((d, 2 * fs), F32),
            pltpu.VMEM((fs, d), F32),
            pltpu.SemaphoreType.DMA((10,)),
            pltpu.SemaphoreType.DMA((3,)),
        ],
        input_output_aliases=alias,
        cost_estimate=pl.CostEstimate(flops=12 * 2 * rows * d * fs, bytes_accessed=14 * 1024 * 1024,
                                      transcendentals=2 * rows * fs),
        name=f"dw{e}{'i' if first else ''}",
    )(*args)


def solution(mesh):
    np_ = mesh.shape['expert']
    tok = P(('data', 'expert'), None)
    buf = P(('data', 'expert'), None, None)
    wsp = P('expert', None, None)

    def body(dy, gates, topk_idx, slot, yd, xd, h1, h3, w1, w3, w2):
        d = dy.shape[1]
        el = w1.shape[0]
        cap = xd.shape[1] // np_
        idx = lax.axis_index('data').astype(jnp.int32).reshape(1)

        def chain(c, e):
            r, l = [c], [c]
            for k in range(4 if e == 0 else 3):
                r.append(lax.ppermute(r[-1], 'data', RIGHT))
            for k in range(3 if e == 0 else 4):
                l.append(lax.ppermute(l[-1], 'data', LEFT))
            return r, l

        xch = [chain(xd[e], e) for e in range(el)]

        v = (gates[:, :, None] * dy.astype(F32)[:, None, :]).astype(BF16)
        col = jnp.where(slot >= 0, slot, cap)
        send = jnp.zeros((np_ * el, cap, d), BF16).at[topk_idx, col].set(v, mode='drop')
        recv = lax.all_to_all(send.reshape(np_, el, cap, d), 'expert', 0, 0, tiled=True)
        dyd = jnp.swapaxes(recv, 0, 1).reshape(el, np_ * cap, d)
        ych = [chain(dyd[e], e) for e in range(el)]
        dg = jnp.einsum('tkd,td->tk', yd, dy, preferred_element_type=F32)

        h1f = h1.astype(F32)
        h3f = h3.astype(F32)
        s = jax.nn.sigmoid(h1f)
        silu = h1f * s
        da = jnp.einsum('ecd,efd->ecf', dyd, w2, preferred_element_type=F32).astype(BF16).astype(F32)
        dh1 = (da * h3f * s * (1.0 + h1f * (1.0 - s))).astype(BF16)
        dh3 = (da * silu).astype(BF16)
        dxd = (jnp.einsum('ecf,edf->ecd', dh1, w1, preferred_element_type=F32)
               + jnp.einsum('ecf,edf->ecd', dh3, w3, preferred_element_type=F32)).astype(BF16)
        out = jnp.swapaxes(dxd.reshape(el, np_, cap, d), 0, 1)
        back = lax.all_to_all(out, 'expert', 0, 0, tiled=True).reshape(np_ * el, cap, d)
        got = back[topk_idx, jnp.minimum(col, cap - 1)].astype(F32)
        dx = jnp.sum(jnp.where((slot >= 0)[:, :, None], got, 0.0), axis=1).astype(BF16)

        acc = None
        seen = [False] * el
        for k in range(4):
            for e in range(el):
                (xr, xl), (yr, yl) = xch[e], ych[e]
                if e == 0:
                    pick = lambda r, l: (l[k], r[k + 1])
                else:
                    pick = lambda r, l: (r[k], l[k + 1])
                acc = _dw_call(e, idx, pick(xr, xl), pick(yr, yl), w1, w3, w2,
                               None if acc is None else (acc if seen[e] else None, acc))
                seen[e] = True
        dw1, dw3, dw2 = acc
        return dx, dg, dw1, dw3, dw2

    return jax.shard_map(body, mesh=mesh,
                         in_specs=(tok, tok, tok, tok, buf, buf, buf, buf, wsp, wsp, wsp),
                         out_specs=(tok, tok, P('expert', None, 'data'), P('expert', None, 'data'), P('expert', 'data', None)),
                         check_vma=False)
```

```python
import functools

import jax
import jax.numpy as jnp
from jax import lax
from jax.experimental import pallas as pl
from jax.experimental.pallas import tpu as pltpu
from jax.sharding import PartitionSpec as P


F32 = jnp.float32
BF16 = jnp.bfloat16


RING = (0, 2, 4, 6, 7, 5, 3, 1)
RIGHT = [(RING[i], RING[(i + 1) % 8]) for i in range(8)]
LEFT = [(RING[(i + 1) % 8], RING[i]) for i in range(8)]


def _dw_kernel(e, n, first, idx_ref, *refs):
    xs, ys = refs[:n], refs[n:2 * n]
    w1, w3, w2 = refs[2 * n:2 * n + 3]
    o1, o3, o2 = refs[-15:-12]
    x, y, w13, w2s, dh, a, acc13, acc2, wsem, xsem, ysem, osem = refs[-12:]
    rows = xs[0].shape[0]
    fs = w2s.shape[0]
    tile = 128
    per = rows // tile
    f0 = pl.multiple_of(idx_ref[0] * fs, 128)
    half = lambda j: pl.ds(j * fs, fs)

    def row_copy(src, dst, j, sem):
        return pltpu.make_async_copy(src, dst.at[pl.ds(pl.multiple_of(j * rows, 128), rows)], sem.at[j])

    wcp = [
        pltpu.make_async_copy(w1.at[e, :, pl.ds(f0, fs)], w13.at[:, half(0)], wsem.at[0]),
        pltpu.make_async_copy(w3.at[e, :, pl.ds(f0, fs)], w13.at[:, half(1)], wsem.at[1]),
        pltpu.make_async_copy(w2.at[e, pl.ds(f0, fs), :], w2s, wsem.at[2]),
    ]
    row_copy(xs[0], x, 0, xsem).start()
    for c in wcp:
        c.start()
    row_copy(ys[0], y, 0, ysem).start()
    for j in range(1, n):
        row_copy(xs[j], x, j, xsem).start()
        row_copy(ys[j], y, j, ysem).start()
    prev = []
    if not first:
        prev = [
            pltpu.make_async_copy(o1.at[e], acc13.at[:, half(0)], wsem.at[3]),
            pltpu.make_async_copy(o3.at[e], acc13.at[:, half(1)], wsem.at[4]),
            pltpu.make_async_copy(o2.at[e], acc2, wsem.at[5]),
        ]
        for c in prev:
            c.start()
    for c in wcp:
        c.wait()

    def rows_body(i, _):
        @pl.when(lax.rem(i, per) == 0)
        def _():
            row_copy(xs[0], x, i // per, xsem).wait()
            row_copy(ys[0], y, i // per, ysem).wait()

        r = pl.ds(pl.multiple_of(i * tile, 128), tile)
        h = jnp.dot(x[r, :], w13[...], preferred_element_type=F32).astype(BF16).astype(F32)
        da = lax.dot_general(y[r, :], w2s[...], (((1,), (1,)), ((), ())),
                             preferred_element_type=F32).astype(BF16).astype(F32)
        h1, h3 = h[:, :fs], h[:, fs:]
        s = jax.nn.sigmoid(h1)
        silu = h1 * s
        a[r, :] = (silu * h3).astype(BF16)
        dh[r, :fs] = (da * h3 * s * (1.0 + h1 * (1.0 - s))).astype(BF16)
        dh[r, fs:] = (da * silu).astype(BF16)
        return 0

    lax.fori_loop(0, per * n, rows_body, 0)
    for c in prev:
        c.wait()

    def acc(ref, m, val):
        if first:
            ref[m, :] = val
        else:
            ref[m, :] += val

    def out_copies(i):
        m = pl.ds(pl.multiple_of(i * 256, 256), 256)
        return (pltpu.make_async_copy(acc13.at[m, half(0)], o1.at[e, m], osem.at[0]),
                pltpu.make_async_copy(acc13.at[m, half(1)], o3.at[e, m], osem.at[1]))

    def d13_body(i, _):
        m = pl.ds(pl.multiple_of(i * 256, 256), 256)
        acc(acc13, m, lax.dot_general(x[:, m], dh[...], (((0,), (0,)), ((), ())), preferred_element_type=F32))
        for c in out_copies(i):
            c.start()
        return 0

    nm = x.shape[1] // 256
    lax.fori_loop(0, nm, d13_body, 0)

    def d2_copy(i):
        m = pl.ds(pl.multiple_of(i * 128, 128), 128)
        return pltpu.make_async_copy(acc2.at[m], o2.at[e, m], osem.at[2])

    def d2_body(i, _):
        m = pl.ds(pl.multiple_of(i * 128, 128), 128)
        acc(acc2, m, lax.dot_general(a[:, m], y[...], (((0,), (0,)), ((), ())), preferred_element_type=F32))
        d2_copy(i).start()
        return 0

    lax.fori_loop(0, fs // 128, d2_body, 0)

    def drain13(i, _):
        for c in out_copies(i):
            c.wait()
        return 0

    def drain2(i, _):
        d2_copy(i).wait()
        return 0

    lax.fori_loop(0, nm, drain13, 0)
    lax.fori_loop(0, fs // 128, drain2, 0)


def _dw_call(e, idx, xs, ys, w1, w3, w2, prev, first):
    el, d, f = w1.shape
    n, rows = len(xs), xs[0].shape[0]
    fs = f // 8
    anyspec = pl.BlockSpec(memory_space=pl.ANY)
    outs = [jax.ShapeDtypeStruct((el, d, fs), F32), jax.ShapeDtypeStruct((el, d, fs), F32),
            jax.ShapeDtypeStruct((el, fs, d), F32)]
    args = [idx, *xs, *ys, w1, w3, w2]
    alias = {}
    if prev is not None:
        alias = {len(args) + i: i for i in range(3)}
        args += list(prev)
    return pl.pallas_call(
        functools.partial(_dw_kernel, e, n, first),
        out_shape=outs,
        in_specs=[pl.BlockSpec(memory_space=pltpu.SMEM)] + [anyspec] * (len(args) - 1),
        out_specs=[anyspec] * 3,
        scratch_shapes=[
            pltpu.VMEM((n * rows, d), BF16),
            pltpu.VMEM((n * rows, d), BF16),
            pltpu.VMEM((d, 2 * fs), BF16),
            pltpu.VMEM((fs, d), BF16),
            pltpu.VMEM((n * rows, 2 * fs), BF16),
            pltpu.VMEM((n * rows, fs), BF16),
            pltpu.VMEM((d, 2 * fs), F32),
            pltpu.VMEM((fs, d), F32),
            pltpu.SemaphoreType.DMA((6,)),
            pltpu.SemaphoreType.DMA((n,)),
            pltpu.SemaphoreType.DMA((n,)),
            pltpu.SemaphoreType.DMA((3,)),
        ],
        input_output_aliases=alias,
        cost_estimate=pl.CostEstimate(flops=12 * n * rows * d * fs, bytes_accessed=n * 2 * 2**20 + 9 * 2**20,
                                      transcendentals=n * rows * fs),
    )(*args)


def solution(mesh):
    np_ = mesh.shape['expert']
    tok = P(('data', 'expert'), None)
    buf = P(('data', 'expert'), None, None)
    wsp = P('expert', None, None)

    def body(dy, gates, topk_idx, slot, yd, xd, h1, h3, w1, w3, w2):
        d = dy.shape[1]
        el = w1.shape[0]
        cap = xd.shape[1] // np_
        idx = lax.axis_index('data').astype(jnp.int32).reshape(1)

        def chain(c, last_right):
            r, l = [c], [c]
            for _ in range(3):
                r.append(lax.ppermute(r[-1], 'data', RIGHT))
                l.append(lax.ppermute(l[-1], 'data', LEFT))
            r.append(lax.ppermute(r[3], 'data', RIGHT) if last_right else lax.ppermute(l[3], 'data', LEFT))
            return r, l

        xch = [chain(xd[e], True) for e in range(el)]

        v = (gates[:, :, None] * dy.astype(F32)[:, None, :]).astype(BF16)
        col = jnp.where(slot >= 0, slot, cap)
        send = jnp.zeros((np_ * el, cap, d), BF16).at[topk_idx, col].set(v, mode='drop')
        recv = lax.all_to_all(send.reshape(np_, el, cap, d), 'expert', 0, 0, tiled=True)
        dyd = jnp.swapaxes(recv, 0, 1).reshape(el, np_ * cap, d)
        ych = [chain(dyd[e], False) for e in range(el)]
        dg = jnp.einsum('tkd,td->tk', yd, dy, preferred_element_type=F32)

        h1f = h1.astype(F32)
        h3f = h3.astype(F32)
        s = jax.nn.sigmoid(h1f)
        silu = h1f * s
        da = jnp.einsum('ecd,efd->ecf', dyd, w2, preferred_element_type=F32).astype(BF16).astype(F32)
        dh1 = (da * h3f * s * (1.0 + h1f * (1.0 - s))).astype(BF16)
        dh3 = (da * silu).astype(BF16)
        dxd = (jnp.einsum('ecf,edf->ecd', dh1, w1, preferred_element_type=F32)
               + jnp.einsum('ecf,edf->ecd', dh3, w3, preferred_element_type=F32)).astype(BF16)
        out = jnp.swapaxes(dxd.reshape(el, np_, cap, d), 0, 1)
        back = lax.all_to_all(out, 'expert', 0, 0, tiled=True).reshape(np_ * el, cap, d)
        got = back[topk_idx, jnp.minimum(col, cap - 1)].astype(F32)
        dx = jnp.sum(jnp.where((slot >= 0)[:, :, None], got, 0.0), axis=1).astype(BF16)

        acc = None
        steps = (lambda r, l: (r[0], r[1]), lambda r, l: (l[1], r[2]),
                 lambda r, l: (l[2], r[3], l[3]), lambda r, l: (r[4],))
        for k, pick in enumerate(steps):
            for e in range(el):
                acc = _dw_call(e, idx, pick(*xch[e]), pick(*ych[e]), w1, w3, w2, acc, k == 0)
        dw1, dw3, dw2 = acc
        return dx, dg, dw1, dw3, dw2

    return jax.shard_map(body, mesh=mesh,
                         in_specs=(tok, tok, tok, tok, buf, buf, buf, buf, wsp, wsp, wsp),
                         out_specs=(tok, tok, P('expert', None, 'data'), P('expert', None, 'data'), P('expert', 'data', None)),
                         check_vma=False)
```

```python
import functools

import jax
import jax.numpy as jnp
from jax import lax
from jax.experimental import pallas as pl
from jax.experimental.pallas import tpu as pltpu
from jax.sharding import PartitionSpec as P


F32 = jnp.float32
BF16 = jnp.bfloat16


PACK = 1024
META = 16
RING = (0, 2, 4, 6, 7, 5, 3, 1)
RIGHT = [(RING[i], RING[(i + 1) % 8]) for i in range(8)]
LEFT = [(RING[(i + 1) % 8], RING[i]) for i in range(8)]


def _pack_kernel(grouped, starts, pos_ref, meta_ref, src_ref, *refs):
    n = len(starts)
    outs, src, sem = refs[:n], refs[n], refs[n + 1]
    cps = []
    if grouped:
        np_, el, cap, _ = src_ref.shape
        for p in range(np_):
            for e in range(el):
                dst = src.at[pl.ds(e * np_ * cap + p * cap, cap)]
                cps.append(pltpu.make_async_copy(src_ref.at[p, e], dst, sem.at[p * el + e]))
    else:
        el, rows, _ = src_ref.shape
        for e in range(el):
            cps.append(pltpu.make_async_copy(src_ref.at[e], src.at[pl.ds(e * rows, rows)], sem.at[e]))
    for c in cps:
        c.start()
    for c in cps:
        c.wait()
    pos = pos_ref[...]
    for o, (base, rows, meta) in zip(outs, starts):
        def tile_body(i, _, o=o, base=base):
            r = pl.multiple_of(i * 128, 128)
            row = (lax.broadcasted_iota(jnp.int32, (128, 1), 0) + (r + base)).astype(F32)
            hot = jnp.where(pos == row, 1.0, 0.0).astype(BF16)
            o[pl.ds(r, 128), :] = jnp.dot(hot, src[...], preferred_element_type=F32).astype(BF16)
            return 0

        lax.fori_loop(0, rows // 128, tile_body, 0)
        if meta:
            k = lax.broadcasted_iota(jnp.int32, (META, o.shape[1]), 0)
            v = jnp.where(k == 0, meta_ref[0], jnp.where(k == 1, meta_ref[1], meta_ref[2]))
            o[pl.ds(rows, META), :] = v.astype(BF16)


def _pack(src, pos, meta, starts):
    d = src.shape[-1]
    rows = pos.shape[1]
    vspec = pl.BlockSpec(memory_space=pltpu.VMEM)
    total = sum(r for _, r, _ in starts)
    return pl.pallas_call(
        functools.partial(_pack_kernel, src.ndim == 4, starts),
        out_shape=[jax.ShapeDtypeStruct((r + META * m, d), BF16) for _, r, m in starts],
        in_specs=[vspec, pl.BlockSpec(memory_space=pltpu.SMEM), pl.BlockSpec(memory_space=pl.ANY)],
        out_specs=[vspec] * len(starts),
        scratch_shapes=[pltpu.VMEM((rows, d), BF16), pltpu.SemaphoreType.DMA((8,))],
        cost_estimate=pl.CostEstimate(flops=2 * total * rows * d, bytes_accessed=2 * (rows + total) * d, transcendentals=0),
    )(pos, meta, src)


def _dwp_kernel(n, first, idx_ref, *refs):
    xc, yc = refs[:2 * n], refs[2 * n:4 * n]
    w1, w3, w2 = refs[4 * n:4 * n + 3]
    o1, o3, o2 = refs[-17:-14]
    x, y, xm, w13, w2s, dh, a, acc13, acc2, wsem, xsem, ysem, msem, osem = refs[-14:]
    el, fs, d = w2s.shape
    hp = PACK // 2
    rows = dh.shape[0] // n
    gap = PACK - rows
    f0 = pl.multiple_of(idx_ref[0] * fs, 128)
    half = lambda j: pl.ds(j * fs, fs)

    def w_copies(e):
        return [pltpu.make_async_copy(w1.at[e, :, pl.ds(f0, fs)], w13.at[e, :, half(0)], wsem.at[0, e]),
                pltpu.make_async_copy(w3.at[e, :, pl.ds(f0, fs)], w13.at[e, :, half(1)], wsem.at[1, e]),
                pltpu.make_async_copy(w2.at[e, pl.ds(f0, fs), :], w2s.at[e], wsem.at[2, e])]

    def prev_copies(e):
        return [pltpu.make_async_copy(o1.at[e], acc13.at[e, :, half(0)], wsem.at[3, e]),
                pltpu.make_async_copy(o3.at[e], acc13.at[e, :, half(1)], wsem.at[4, e]),
                pltpu.make_async_copy(o2.at[e], acc2.at[e], wsem.at[5, e])]

    def row_copies(c, s, refs_s):
        lo, hi = refs_s
        at = lambda k: pl.ds(pl.multiple_of(s * PACK + k * hp, 128), hp)
        sem = xsem if c is x else ysem
        cps = [pltpu.make_async_copy(lo.at[pl.ds(0, hp)], c.at[at(0)], sem.at[0, s]),
               pltpu.make_async_copy(hi, c.at[at(1)], sem.at[1, s])]
        if c is x:
            cps.append(pltpu.make_async_copy(lo.at[pl.ds(hp, META)], xm.at[pl.ds(pl.multiple_of(s * META, META), META)], msem.at[s]))
        return cps

    for c in w_copies(0):
        c.start()
    for s in range(n):
        for c in row_copies(x, s, xc[2 * s:2 * s + 2]) + row_copies(y, s, yc[2 * s:2 * s + 2]):
            c.start()
    for c in w_copies(1):
        c.start()
    if not first:
        for e in range(el):
            for c in prev_copies(e):
                c.start()

    per = rows // 128

    def expert_body(e, _):
        off = e * gap
        sign = (1 - 2 * e).astype(F32)
        for c in w_copies(e):
            c.wait()

        def rows_body(i, _):
            s = i // per
            t = i - s * per

            @pl.when((e == 0) & (t == 0))
            def _():
                for c in row_copies(x, s, xc[:2]) + row_copies(y, s, yc[:2]):
                    c.wait()

            r = pl.ds(pl.multiple_of(s * PACK + off + t * 128, 128), 128)
            m = xm[pl.ds(pl.multiple_of(s * META, META), META), :fs].astype(F32)
            cut = m[0:1, :] * 8.0 + m[1:2, :]
            row = (lax.broadcasted_iota(jnp.int32, (128, fs), 0) + (off + t * 128)).astype(F32)
            keep = (cut - row - 0.5) * sign > 0.0
            h = jnp.dot(x[r, :], w13[e], preferred_element_type=F32).astype(BF16).astype(F32)
            da = lax.dot_general(y[r, :], w2s[e], (((1,), (1,)), ((), ())),
                                 preferred_element_type=F32).astype(BF16).astype(F32)
            h1 = jnp.where(keep, h[:, :fs], 0.0)
            h3 = jnp.where(keep, h[:, fs:], 0.0)
            da = jnp.where(keep, da, 0.0)
            sg = jax.nn.sigmoid(h1)
            silu = h1 * sg
            o = pl.ds(pl.multiple_of(i * 128, 128), 128)
            a[o, :] = (silu * h3).astype(BF16)
            dh[o, :fs] = (da * h3 * sg * (1.0 + h1 * (1.0 - sg))).astype(BF16)
            dh[o, fs:] = (da * silu).astype(BF16)
            return 0

        lax.fori_loop(0, per * n, rows_body, 0)
        if not first:
            for c in prev_copies(e):
                c.wait()

        def win(ref, s, cols):
            return ref[pl.ds(pl.multiple_of(s * PACK + off, 128), rows), cols]

        def acc(ref, m, parts):
            val = parts[0]
            for p in parts[1:]:
                val = val + p
            if first:
                ref[e, m, :] = val
            else:
                ref[e, m, :] += val

        def d13_body(i, _):
            m = pl.ds(pl.multiple_of(i * 128, 128), 128)
            acc(acc13, m, [lax.dot_general(win(x, s, m), dh[s * rows:(s + 1) * rows, :], (((0,), (0,)), ((), ())),
                                           preferred_element_type=F32) for s in range(n)])
            pltpu.make_async_copy(acc13.at[e, m, half(0)], o1.at[e, m], osem.at[0]).start()
            pltpu.make_async_copy(acc13.at[e, m, half(1)], o3.at[e, m], osem.at[1]).start()
            return 0

        lax.fori_loop(0, d // 128, d13_body, 0)

        def d2_body(i, _):
            m = pl.ds(pl.multiple_of(i * 128, 128), 128)
            acc(acc2, m, [lax.dot_general(a[s * rows:(s + 1) * rows, m], win(y, s, slice(None)), (((0,), (0,)), ((), ())),
                                          preferred_element_type=F32) for s in range(n)])
            pltpu.make_async_copy(acc2.at[e, m], o2.at[e, m], osem.at[2]).start()
            return 0

        lax.fori_loop(0, fs // 128, d2_body, 0)
        return 0

    lax.fori_loop(0, el, expert_body, 0)
    for e in range(el):
        pltpu.make_async_copy(acc13.at[e, :, half(0)], o1.at[e], osem.at[0]).wait()
        pltpu.make_async_copy(acc13.at[e, :, half(1)], o3.at[e], osem.at[1]).wait()
        pltpu.make_async_copy(acc2.at[e], o2.at[e], osem.at[2]).wait()


def _dwp_call(idx, xs, ys, rows, w1, w3, w2, prev):
    el, d, f = w1.shape
    n = len(xs)
    fs = f // 8
    anyspec = pl.BlockSpec(memory_space=pl.ANY)
    outs = [jax.ShapeDtypeStruct((el, d, fs), F32), jax.ShapeDtypeStruct((el, d, fs), F32),
            jax.ShapeDtypeStruct((el, fs, d), F32)]
    args = [idx, *(c for p in xs for c in p), *(c for p in ys for c in p), w1, w3, w2]
    alias = {}
    if prev is not None:
        alias = {len(args) + i: i for i in range(3)}
        args += list(prev)
    return pl.pallas_call(
        functools.partial(_dwp_kernel, n, prev is None),
        out_shape=outs,
        in_specs=[pl.BlockSpec(memory_space=pltpu.SMEM)] + [anyspec] * (len(args) - 1),
        out_specs=[anyspec] * 3,
        scratch_shapes=[
            pltpu.VMEM((n * PACK, d), BF16),
            pltpu.VMEM((n * PACK, d), BF16),
            pltpu.VMEM((n * META, d), BF16),
            pltpu.VMEM((el, d, 2 * fs), BF16),
            pltpu.VMEM((el, fs, d), BF16),
            pltpu.VMEM((n * rows, 2 * fs), BF16),
            pltpu.VMEM((n * rows, fs), BF16),
            pltpu.VMEM((el, d, 2 * fs), F32),
            pltpu.VMEM((el, fs, d), F32),
            pltpu.SemaphoreType.DMA((6, el)),
            pltpu.SemaphoreType.DMA((2, n)),
            pltpu.SemaphoreType.DMA((2, n)),
            pltpu.SemaphoreType.DMA((n,)),
            pltpu.SemaphoreType.DMA((3,)),
        ],
        input_output_aliases=alias,
        cost_estimate=pl.CostEstimate(flops=24 * n * rows * d * fs, bytes_accessed=n * 4 * 2**20 + 18 * 2**20,
                                      transcendentals=2 * n * rows * fs),
    )(*args)


def _dw_kernel(e, n, first, idx_ref, *refs):
    xs, ys = refs[:n], refs[n:2 * n]
    w1, w3, w2 = refs[2 * n:2 * n + 3]
    o1, o3, o2 = refs[-15:-12]
    x, y, w13, w2s, dh, a, acc13, acc2, wsem, xsem, ysem, osem = refs[-12:]
    rows = xs[0].shape[0]
    fs = w2s.shape[0]
    tile = 128
    per = rows // tile
    f0 = pl.multiple_of(idx_ref[0] * fs, 128)
    half = lambda j: pl.ds(j * fs, fs)

    def row_copy(src, dst, j, sem):
        return pltpu.make_async_copy(src, dst.at[pl.ds(pl.multiple_of(j * rows, 128), rows)], sem.at[j])

    wcp = [
        pltpu.make_async_copy(w1.at[e, :, pl.ds(f0, fs)], w13.at[:, half(0)], wsem.at[0]),
        pltpu.make_async_copy(w3.at[e, :, pl.ds(f0, fs)], w13.at[:, half(1)], wsem.at[1]),
        pltpu.make_async_copy(w2.at[e, pl.ds(f0, fs), :], w2s, wsem.at[2]),
    ]
    row_copy(xs[0], x, 0, xsem).start()
    for c in wcp:
        c.start()
    row_copy(ys[0], y, 0, ysem).start()
    for j in range(1, n):
        row_copy(xs[j], x, j, xsem).start()
        row_copy(ys[j], y, j, ysem).start()
    prev = []
    if not first:
        prev = [
            pltpu.make_async_copy(o1.at[e], acc13.at[:, half(0)], wsem.at[3]),
            pltpu.make_async_copy(o3.at[e], acc13.at[:, half(1)], wsem.at[4]),
            pltpu.make_async_copy(o2.at[e], acc2, wsem.at[5]),
        ]
        for c in prev:
            c.start()
    for c in wcp:
        c.wait()

    def rows_body(i, _):
        @pl.when(lax.rem(i, per) == 0)
        def _():
            row_copy(xs[0], x, i // per, xsem).wait()
            row_copy(ys[0], y, i // per, ysem).wait()

        r = pl.ds(pl.multiple_of(i * tile, 128), tile)
        h = jnp.dot(x[r, :], w13[...], preferred_element_type=F32).astype(BF16).astype(F32)
        da = lax.dot_general(y[r, :], w2s[...], (((1,), (1,)), ((), ())),
                             preferred_element_type=F32).astype(BF16).astype(F32)
        h1, h3 = h[:, :fs], h[:, fs:]
        s = jax.nn.sigmoid(h1)
        silu = h1 * s
        a[r, :] = (silu * h3).astype(BF16)
        dh[r, :fs] = (da * h3 * s * (1.0 + h1 * (1.0 - s))).astype(BF16)
        dh[r, fs:] = (da * silu).astype(BF16)
        return 0

    lax.fori_loop(0, per * n, rows_body, 0)
    for c in prev:
        c.wait()

    def acc(ref, m, val):
        if first:
            ref[m, :] = val
        else:
            ref[m, :] += val

    def out_copies(i):
        m = pl.ds(pl.multiple_of(i * 256, 256), 256)
        return (pltpu.make_async_copy(acc13.at[m, half(0)], o1.at[e, m], osem.at[0]),
                pltpu.make_async_copy(acc13.at[m, half(1)], o3.at[e, m], osem.at[1]))

    def d13_body(i, _):
        m = pl.ds(pl.multiple_of(i * 256, 256), 256)
        acc(acc13, m, lax.dot_general(x[:, m], dh[...], (((0,), (0,)), ((), ())), preferred_element_type=F32))
        for c in out_copies(i):
            c.start()
        return 0

    nm = x.shape[1] // 256
    lax.fori_loop(0, nm, d13_body, 0)

    def d2_copy(i):
        m = pl.ds(pl.multiple_of(i * 128, 128), 128)
        return pltpu.make_async_copy(acc2.at[m], o2.at[e, m], osem.at[2])

    def d2_body(i, _):
        m = pl.ds(pl.multiple_of(i * 128, 128), 128)
        acc(acc2, m, lax.dot_general(a[:, m], y[...], (((0,), (0,)), ((), ())), preferred_element_type=F32))
        d2_copy(i).start()
        return 0

    lax.fori_loop(0, fs // 128, d2_body, 0)

    def drain13(i, _):
        for c in out_copies(i):
            c.wait()
        return 0

    def drain2(i, _):
        d2_copy(i).wait()
        return 0

    lax.fori_loop(0, nm, drain13, 0)
    lax.fori_loop(0, fs // 128, drain2, 0)


def _dw_call(e, idx, xs, ys, w1, w3, w2, prev, first):
    el, d, f = w1.shape
    n, rows = len(xs), xs[0].shape[0]
    fs = f // 8
    anyspec = pl.BlockSpec(memory_space=pl.ANY)
    outs = [jax.ShapeDtypeStruct((el, d, fs), F32), jax.ShapeDtypeStruct((el, d, fs), F32),
            jax.ShapeDtypeStruct((el, fs, d), F32)]
    args = [idx, *xs, *ys, w1, w3, w2]
    alias = {}
    if prev is not None:
        alias = {len(args) + i: i for i in range(3)}
        args += list(prev)
    return pl.pallas_call(
        functools.partial(_dw_kernel, e, n, first),
        out_shape=outs,
        in_specs=[pl.BlockSpec(memory_space=pltpu.SMEM)] + [anyspec] * (len(args) - 1),
        out_specs=[anyspec] * 3,
        scratch_shapes=[
            pltpu.VMEM((n * rows, d), BF16),
            pltpu.VMEM((n * rows, d), BF16),
            pltpu.VMEM((d, 2 * fs), BF16),
            pltpu.VMEM((fs, d), BF16),
            pltpu.VMEM((n * rows, 2 * fs), BF16),
            pltpu.VMEM((n * rows, fs), BF16),
            pltpu.VMEM((d, 2 * fs), F32),
            pltpu.VMEM((fs, d), F32),
            pltpu.SemaphoreType.DMA((6,)),
            pltpu.SemaphoreType.DMA((n,)),
            pltpu.SemaphoreType.DMA((n,)),
            pltpu.SemaphoreType.DMA((3,)),
        ],
        input_output_aliases=alias,
        cost_estimate=pl.CostEstimate(flops=12 * n * rows * d * fs, bytes_accessed=n * 2 * 2**20 + 9 * 2**20,
                                      transcendentals=n * rows * fs),
    )(*args)


def solution(mesh):
    np_ = mesh.shape['expert']
    tok = P(('data', 'expert'), None)
    buf = P(('data', 'expert'), None, None)
    wsp = P('expert', None, None)

    def body(dy, gates, topk_idx, slot, yd, xd, h1, h3, w1, w3, w2):
        d = dy.shape[1]
        el = w1.shape[0]
        cap = xd.shape[1] // np_
        idx = lax.axis_index('data').astype(jnp.int32).reshape(1)

        used = (jnp.max(jnp.abs(xd.astype(F32)), axis=-1) > 0.0).astype(BF16)
        rows = xd.shape[1]
        at = lax.broadcasted_iota(jnp.int32, (rows, rows), 0)
        to = lax.broadcasted_iota(jnp.int32, (rows, rows), 1)
        rank = jnp.dot(used, (at < to).astype(BF16), preferred_element_type=F32)
        count = jnp.sum(used.astype(F32), axis=1)
        room = PACK - count[0]
        back = jnp.where(rank[1] < room, PACK - 1 - rank[1], PACK + rank[1] - room)
        pos = jnp.where(used > 0, jnp.stack([rank[0], back]), -1.0).reshape(1, el * rows)
        cut = jnp.stack([jnp.floor(count[0] / 8.0), count[0] - 8.0 * jnp.floor(count[0] / 8.0)])
        halves = ((0, PACK // 2, True), (PACK // 2, PACK // 2, False))

        def chain(c, last_right):
            r, l = [c], [c]
            for _ in range(3):
                r.append([lax.ppermute(v, 'data', RIGHT) for v in r[-1]])
                l.append([lax.ppermute(v, 'data', LEFT) for v in l[-1]])
            perm, last = (RIGHT, r[3]) if last_right else (LEFT, l[3])
            r.append([lax.ppermute(v, 'data', perm) for v in last])
            return r, l

        xr, xl = chain(_pack(xd, pos, jnp.append(cut, 0.0), halves), True)
        over = lax.pmax((count[0] + count[1] > PACK).astype(F32), 'expert')

        v = (gates[:, :, None] * dy.astype(F32)[:, None, :]).astype(BF16)
        col = jnp.where(slot >= 0, slot, cap)
        send = jnp.zeros((np_ * el, cap, d), BF16).at[topk_idx, col].set(v, mode='drop')
        recv = lax.all_to_all(send.reshape(np_, el, cap, d), 'expert', 0, 0, tiled=True)
        dyd = jnp.swapaxes(recv, 0, 1).reshape(el, np_ * cap, d)
        yr, yl = chain(_pack(recv, pos, jnp.stack([over, over, over]), halves), False)
        dg = jnp.einsum('tkd,td->tk', yd, dy, preferred_element_type=F32)

        h1f = h1.astype(F32)
        h3f = h3.astype(F32)
        s = jax.nn.sigmoid(h1f)
        silu = h1f * s
        da = jnp.einsum('ecd,efd->ecf', dyd, w2, preferred_element_type=F32).astype(BF16).astype(F32)
        dh1 = (da * h3f * s * (1.0 + h1f * (1.0 - s))).astype(BF16)
        dh3 = (da * silu).astype(BF16)
        dxd = (jnp.einsum('ecf,edf->ecd', dh1, w1, preferred_element_type=F32)
               + jnp.einsum('ecf,edf->ecd', dh3, w3, preferred_element_type=F32)).astype(BF16)
        out = jnp.swapaxes(dxd.reshape(el, np_, cap, d), 0, 1)
        back = lax.all_to_all(out, 'expert', 0, 0, tiled=True).reshape(np_ * el, cap, d)
        got = back[topk_idx, jnp.minimum(col, cap - 1)].astype(F32)
        dx = jnp.sum(jnp.where((slot >= 0)[:, :, None], got, 0.0), axis=1).astype(BF16)

        acc = None
        for pick in (lambda r, l: (r[0], r[1], l[1]), lambda r, l: (r[2], l[2]),
                     lambda r, l: (r[3], l[3]), lambda r, l: (r[4],)):
            acc = _dwp_call(idx, pick(xr, xl), pick(yr, yl), rows, w1, w3, w2, acc)

        flags = [c[0][PACK // 2, 0] for c in yr + yl[1:]]
        some = functools.reduce(jnp.maximum, flags) > 0
        rest = ((PACK, el * rows - PACK, False),)

        def spill(acc):
            zero = jnp.zeros(3, F32)
            xo, = _pack(xd, pos, zero, rest)
            yo, = _pack(recv, pos, zero, rest)

            def hop(_, st):
                xo, yo, acc = st
                acc = _dw_call(1, idx, [xo], [yo], w1, w3, w2, acc, False)
                return lax.ppermute(xo, 'data', RIGHT), lax.ppermute(yo, 'data', RIGHT), tuple(acc)

            return lax.fori_loop(0, 8, hop, (xo, yo, acc))[2]

        acc = lax.cond(some, spill, lambda acc: acc, tuple(acc))
        dw1, dw3, dw2 = acc
        return dx, dg, dw1, dw3, dw2

    return jax.shard_map(body, mesh=mesh,
                         in_specs=(tok, tok, tok, tok, buf, buf, buf, buf, wsp, wsp, wsp),
                         out_specs=(tok, tok, P('expert', None, 'data'), P('expert', None, 'data'), P('expert', 'data', None)),
                         check_vma=False)
```

```python
import functools

import jax
import jax.numpy as jnp
from jax import lax
from jax.experimental import pallas as pl
from jax.experimental.pallas import tpu as pltpu
from jax.sharding import PartitionSpec as P


F32 = jnp.float32
BF16 = jnp.bfloat16


PACK = 1024
META = 16
TILE = 256
RING = (0, 2, 4, 6, 7, 5, 3, 1)
RIGHT = [(RING[i], RING[(i + 1) % 8]) for i in range(8)]
LEFT = [(RING[(i + 1) % 8], RING[i]) for i in range(8)]


def _pack_kernel(grouped, el, starts, pos_ref, meta_ref, src_ref, *refs):
    n = len(starts)
    outs, src, fl, sem = refs[:n], refs[n], refs[n + 1], refs[n + 2]
    cps = []
    if grouped:
        np_ = src_ref.shape[0]
        cap = (src_ref.shape[1] - META) // el
        for p in range(np_):
            for e in range(el):
                dst = src.at[pl.ds(e * np_ * cap + p * cap, cap)]
                cps.append(pltpu.make_async_copy(src_ref.at[p, pl.ds(e * cap, cap)], dst, sem.at[p * el + e]))
            cps.append(pltpu.make_async_copy(src_ref.at[p, pl.ds(el * cap, META)], fl.at[pl.ds(p * META, META)],
                                             sem.at[np_ * el + p]))
    else:
        rows = src_ref.shape[1]
        for e in range(el):
            cps.append(pltpu.make_async_copy(src_ref.at[e], src.at[pl.ds(e * rows, rows)], sem.at[e]))
    for c in cps:
        c.start()
    for c in cps:
        c.wait()
    pos = pos_ref[...]
    for o, (base, rows, meta) in zip(outs, starts):
        def tile_body(i, _, o=o, base=base):
            r = pl.multiple_of(i * 128, 128)
            row = (lax.broadcasted_iota(jnp.int32, (128, 1), 0) + (r + base)).astype(F32)
            hot = jnp.where(pos == row, 1.0, 0.0).astype(BF16)
            o[pl.ds(r, 128), :] = jnp.dot(hot, src[...], preferred_element_type=F32).astype(BF16)
            return 0

        lax.fori_loop(0, rows // 128, tile_body, 0)
        if meta and grouped:
            v = fl[pl.ds(0, META), :].astype(F32)
            for p in range(1, np_):
                v = jnp.maximum(v, fl[pl.ds(p * META, META), :].astype(F32))
            o[pl.ds(rows, META), :] = v.astype(BF16)
        elif meta:
            k = lax.broadcasted_iota(jnp.int32, (META, o.shape[1]), 0)
            v = jnp.where(k == 0, meta_ref[0], jnp.where(k == 1, meta_ref[1], jnp.where(k == 2, meta_ref[2], meta_ref[3])))
            o[pl.ds(rows, META), :] = v.astype(BF16)


def _pack(src, pos, meta, starts, el, grouped):
    d = src.shape[-1]
    rows = pos.shape[1]
    vspec = pl.BlockSpec(memory_space=pltpu.VMEM)
    total = sum(r for _, r, _ in starts)
    return pl.pallas_call(
        functools.partial(_pack_kernel, grouped, el, starts),
        out_shape=[jax.ShapeDtypeStruct((r + META * m, d), BF16) for _, r, m in starts],
        in_specs=[vspec, pl.BlockSpec(memory_space=pltpu.SMEM), pl.BlockSpec(memory_space=pl.ANY)],
        out_specs=[vspec] * len(starts),
        scratch_shapes=[pltpu.VMEM((rows, d), BF16), pltpu.VMEM((4 * META, d), BF16), pltpu.SemaphoreType.DMA((12,))],
        cost_estimate=pl.CostEstimate(flops=2 * total * rows * d, bytes_accessed=2 * (rows + total) * d, transcendentals=0),
    )(pos, meta, src)


def _send_kernel(blk, over_ref, to_ref, v_ref, o_ref):
    rows = o_ref.shape[0] // 8

    def tile_body(i, _):
        r = pl.multiple_of(i * rows, 8)
        line = lax.broadcasted_iota(jnp.int32, (rows, v_ref.shape[0]), 0) + r
        hot = jnp.where(to_ref[...] == line, 1.0, 0.0).astype(BF16)
        o_ref[pl.ds(r, rows), :] = jnp.dot(hot, v_ref[...], preferred_element_type=F32).astype(BF16)
        return 0

    lax.fori_loop(0, 8, tile_body, 0)
    for b in range(o_ref.shape[0] // blk):
        o_ref[pl.ds((b + 1) * blk - META, META), :] = jnp.full((META, o_ref.shape[1]), over_ref[0], F32).astype(BF16)


def _send(to, over, v, np_, blk):
    t, d = v.shape
    vspec = pl.BlockSpec(memory_space=pltpu.VMEM)
    return pl.pallas_call(
        functools.partial(_send_kernel, blk),
        out_shape=jax.ShapeDtypeStruct((np_ * blk, d), BF16),
        in_specs=[pl.BlockSpec(memory_space=pltpu.SMEM), vspec, vspec],
        out_specs=vspec,
        cost_estimate=pl.CostEstimate(flops=2 * t * np_ * blk * d, bytes_accessed=2 * (t + np_ * blk) * d, transcendentals=0),
        name="send",
    )(over, to, v)


def _unpack_kernel(at_ref, src_ref, o_ref):
    def tile_body(i, _):
        r = pl.ds(pl.multiple_of(i * 128, 128), 128)
        lane = lax.broadcasted_iota(jnp.int32, (128, src_ref.shape[0]), 1)
        hot = jnp.where(at_ref[r, :] == lane, 1.0, 0.0).astype(BF16)
        o_ref[r, :] = jnp.dot(hot, src_ref[...], preferred_element_type=F32).astype(BF16)
        return 0

    lax.fori_loop(0, o_ref.shape[0] // 128, tile_body, 0)


def _unpack(at, src):
    t, (rows, d) = at.shape[0], src.shape
    vspec = pl.BlockSpec(memory_space=pltpu.VMEM)
    return pl.pallas_call(
        _unpack_kernel,
        out_shape=jax.ShapeDtypeStruct((t, d), BF16),
        in_specs=[vspec, vspec],
        out_specs=vspec,
        cost_estimate=pl.CostEstimate(flops=2 * t * rows * d, bytes_accessed=2 * (rows + t) * d, transcendentals=0),
        name="unpack",
    )(at, src)


def _dwp_kernel(n, first, idx_ref, *refs):
    xc, yc = refs[:2 * n], refs[2 * n:4 * n]
    w1, w3, w2 = refs[4 * n:4 * n + 3]
    o1, o3, o2, oflag = refs[-19:-15]
    x, y, xm, ym, w13, w2s, dh, a, acc13, acc2, wsem, xsem, ysem, msem, osem = refs[-15:]
    el, fs, d = w2s.shape
    hp = PACK // 2
    f0 = pl.multiple_of(idx_ref[0] * fs, 128)
    half = lambda j: pl.ds(j * fs, fs)

    def w_copies(e):
        return [pltpu.make_async_copy(w1.at[e, :, pl.ds(f0, fs)], w13.at[e, :, half(0)], wsem.at[0, e]),
                pltpu.make_async_copy(w3.at[e, :, pl.ds(f0, fs)], w13.at[e, :, half(1)], wsem.at[1, e]),
                pltpu.make_async_copy(w2.at[e, pl.ds(f0, fs), :], w2s.at[e], wsem.at[2, e])]

    def prev_copies(e):
        return [pltpu.make_async_copy(o1.at[e], acc13.at[e, :, half(0)], wsem.at[3, e]),
                pltpu.make_async_copy(o3.at[e], acc13.at[e, :, half(1)], wsem.at[4, e]),
                pltpu.make_async_copy(o2.at[e], acc2.at[e], wsem.at[5, e])]

    def row_copies(s, xp, yp):
        at = lambda k: pl.ds(pl.multiple_of(s * PACK + k * hp, 128), hp)
        mt = pl.ds(pl.multiple_of(s * META, META), META)
        return [pltpu.make_async_copy(xp[0].at[pl.ds(hp, META)], xm.at[mt], msem.at[0, s]),
                pltpu.make_async_copy(yp[0].at[pl.ds(hp, META)], ym.at[mt], msem.at[1, s]),
                pltpu.make_async_copy(xp[0].at[pl.ds(0, hp)], x.at[at(0)], xsem.at[0, s]),
                pltpu.make_async_copy(yp[0].at[pl.ds(0, hp)], y.at[at(0)], ysem.at[0, s]),
                pltpu.make_async_copy(xp[1], x.at[at(1)], xsem.at[1, s]),
                pltpu.make_async_copy(yp[1], y.at[at(1)], ysem.at[1, s])]

    def out_copies(e):
        return [pltpu.make_async_copy(acc13.at[e, :, half(0)], o1.at[e], osem.at[0, e]),
                pltpu.make_async_copy(acc13.at[e, :, half(1)], o3.at[e], osem.at[1, e]),
                pltpu.make_async_copy(acc2.at[e], o2.at[e], osem.at[2, e])]

    for c in w_copies(0):
        c.start()
    for s in range(n):
        for c in row_copies(s, xc[2 * s:2 * s + 2], yc[2 * s:2 * s + 2]):
            c.start()
        if s == 0 and not first:
            for c in prev_copies(0):
                c.start()
    for c in w_copies(1):
        c.start()
    if first:
        acc13[...] = jnp.zeros_like(acc13)
        acc2[...] = jnp.zeros_like(acc2)
    else:
        for c in prev_copies(1):
            c.start()

    def expert_body(e, _):
        sign = (1 - 2 * e).astype(F32)
        for c in w_copies(e):
            c.wait()
        if not first:
            for c in prev_copies(e):
                c.wait()

        def group_body(s, _):
            @pl.when(e == 0)
            def _():
                for c in row_copies(s, xc[:2], yc[:2]):
                    c.wait()

            m = xm[pl.ds(pl.multiple_of(s * META, META), META), :128].astype(F32)
            cut = jnp.max(m[0:1, :] * 8.0 + m[1:2, :])
            other = jnp.max(m[2:3, :] * 8.0 + m[3:4, :])
            used = jnp.where(e == 0, cut, other).astype(jnp.int32)

            def tile_body(k, _):
                base = jnp.where(e == 0, k * TILE, PACK - TILE - k * TILE)
                r = pl.ds(pl.multiple_of(s * PACK + base, TILE), TILE)
                row = (lax.broadcasted_iota(jnp.int32, (TILE, fs), 0) + base).astype(F32)
                keep = (cut - row - 0.5) * sign > 0.0
                h = jnp.dot(x[r, :], w13[e], preferred_element_type=F32).astype(BF16).astype(F32)
                da = lax.dot_general(y[r, :], w2s[e], (((1,), (1,)), ((), ())),
                                     preferred_element_type=F32).astype(BF16).astype(F32)
                h1 = jnp.where(keep, h[:, :fs], 0.0)
                h3 = jnp.where(keep, h[:, fs:], 0.0)
                da = jnp.where(keep, da, 0.0)
                sg = jax.nn.sigmoid(h1)
                silu = h1 * sg
                a[...] = (silu * h3).astype(BF16)
                dh[:, :fs] = (da * h3 * sg * (1.0 + h1 * (1.0 - sg))).astype(BF16)
                dh[:, fs:] = (da * silu).astype(BF16)
                for i in range(d // 256):
                    m = slice(i * 256, (i + 1) * 256)
                    acc13[e, m, :] += lax.dot_general(x[r, m], dh[...], (((0,), (0,)), ((), ())), preferred_element_type=F32)
                acc2[e] += lax.dot_general(a[...], y[r, :], (((0,), (0,)), ((), ())), preferred_element_type=F32)
                return 0

            lax.fori_loop(0, (used + (TILE - 1)) // TILE, tile_body, 0)
            return 0

        lax.fori_loop(0, n, group_body, 0)
        for c in out_copies(e):
            c.start()
        return 0

    lax.fori_loop(0, el, expert_body, 0)
    flag = ym[pl.ds(0, META), :].astype(F32)
    for s in range(1, n):
        flag = jnp.maximum(flag, ym[pl.ds(s * META, META), :].astype(F32))
    if not first:
        flag = jnp.maximum(flag, refs[4 * n + 6][...])
    oflag[...] = flag
    for e in range(el):
        for c in out_copies(e):
            c.wait()


def _dwp_call(idx, xs, ys, w1, w3, w2, prev):
    el, d, f = w1.shape
    n = len(xs)
    fs = f // 8
    anyspec = pl.BlockSpec(memory_space=pl.ANY)
    vspec = pl.BlockSpec(memory_space=pltpu.VMEM)
    outs = [jax.ShapeDtypeStruct((el, d, fs), F32), jax.ShapeDtypeStruct((el, d, fs), F32),
            jax.ShapeDtypeStruct((el, fs, d), F32), jax.ShapeDtypeStruct((META, d), F32)]
    args = [idx, *(c for p in xs for c in p), *(c for p in ys for c in p), w1, w3, w2]
    specs = [pl.BlockSpec(memory_space=pltpu.SMEM)] + [anyspec] * (len(args) - 1)
    alias = {}
    if prev is not None:
        alias = {len(args) + i: i for i in range(3)}
        args += list(prev)
        specs += [anyspec] * 3 + [vspec]
    return pl.pallas_call(
        functools.partial(_dwp_kernel, n, prev is None),
        out_shape=outs,
        in_specs=specs,
        out_specs=[anyspec] * 3 + [vspec],
        scratch_shapes=[
            pltpu.VMEM((n * PACK, d), BF16),
            pltpu.VMEM((n * PACK, d), BF16),
            pltpu.VMEM((n * META, d), BF16),
            pltpu.VMEM((n * META, d), BF16),
            pltpu.VMEM((el, d, 2 * fs), BF16),
            pltpu.VMEM((el, fs, d), BF16),
            pltpu.VMEM((TILE, 2 * fs), BF16),
            pltpu.VMEM((TILE, fs), BF16),
            pltpu.VMEM((el, d, 2 * fs), F32),
            pltpu.VMEM((el, fs, d), F32),
            pltpu.SemaphoreType.DMA((6, el)),
            pltpu.SemaphoreType.DMA((2, n)),
            pltpu.SemaphoreType.DMA((2, n)),
            pltpu.SemaphoreType.DMA((2, n)),
            pltpu.SemaphoreType.DMA((3, el)),
        ],
        input_output_aliases=alias,
        cost_estimate=pl.CostEstimate(flops=12 * n * PACK * d * fs, bytes_accessed=n * 4 * 2**20 + 18 * 2**20,
                                      transcendentals=n * PACK * fs),
    )(*args)


def _dw_kernel(e, n, first, idx_ref, *refs):
    xs, ys = refs[:n], refs[n:2 * n]
    w1, w3, w2 = refs[2 * n:2 * n + 3]
    o1, o3, o2 = refs[-15:-12]
    x, y, w13, w2s, dh, a, acc13, acc2, wsem, xsem, ysem, osem = refs[-12:]
    rows = xs[0].shape[0]
    fs = w2s.shape[0]
    tile = 128
    per = rows // tile
    f0 = pl.multiple_of(idx_ref[0] * fs, 128)
    half = lambda j: pl.ds(j * fs, fs)

    def row_copy(src, dst, j, sem):
        return pltpu.make_async_copy(src, dst.at[pl.ds(pl.multiple_of(j * rows, 128), rows)], sem.at[j])

    wcp = [
        pltpu.make_async_copy(w1.at[e, :, pl.ds(f0, fs)], w13.at[:, half(0)], wsem.at[0]),
        pltpu.make_async_copy(w3.at[e, :, pl.ds(f0, fs)], w13.at[:, half(1)], wsem.at[1]),
        pltpu.make_async_copy(w2.at[e, pl.ds(f0, fs), :], w2s, wsem.at[2]),
    ]
    row_copy(xs[0], x, 0, xsem).start()
    for c in wcp:
        c.start()
    row_copy(ys[0], y, 0, ysem).start()
    for j in range(1, n):
        row_copy(xs[j], x, j, xsem).start()
        row_copy(ys[j], y, j, ysem).start()
    prev = []
    if not first:
        prev = [
            pltpu.make_async_copy(o1.at[e], acc13.at[:, half(0)], wsem.at[3]),
            pltpu.make_async_copy(o3.at[e], acc13.at[:, half(1)], wsem.at[4]),
            pltpu.make_async_copy(o2.at[e], acc2, wsem.at[5]),
        ]
        for c in prev:
            c.start()
    for c in wcp:
        c.wait()

    def rows_body(i, _):
        @pl.when(lax.rem(i, per) == 0)
        def _():
            row_copy(xs[0], x, i // per, xsem).wait()
            row_copy(ys[0], y, i // per, ysem).wait()

        r = pl.ds(pl.multiple_of(i * tile, 128), tile)
        h = jnp.dot(x[r, :], w13[...], preferred_element_type=F32).astype(BF16).astype(F32)
        da = lax.dot_general(y[r, :], w2s[...], (((1,), (1,)), ((), ())),
                             preferred_element_type=F32).astype(BF16).astype(F32)
        h1, h3 = h[:, :fs], h[:, fs:]
        s = jax.nn.sigmoid(h1)
        silu = h1 * s
        a[r, :] = (silu * h3).astype(BF16)
        dh[r, :fs] = (da * h3 * s * (1.0 + h1 * (1.0 - s))).astype(BF16)
        dh[r, fs:] = (da * silu).astype(BF16)
        return 0

    lax.fori_loop(0, per * n, rows_body, 0)
    for c in prev:
        c.wait()

    def acc(ref, m, val):
        if first:
            ref[m, :] = val
        else:
            ref[m, :] += val

    def out_copies(i):
        m = pl.ds(pl.multiple_of(i * 256, 256), 256)
        return (pltpu.make_async_copy(acc13.at[m, half(0)], o1.at[e, m], osem.at[0]),
                pltpu.make_async_copy(acc13.at[m, half(1)], o3.at[e, m], osem.at[1]))

    def d13_body(i, _):
        m = pl.ds(pl.multiple_of(i * 256, 256), 256)
        acc(acc13, m, lax.dot_general(x[:, m], dh[...], (((0,), (0,)), ((), ())), preferred_element_type=F32))
        for c in out_copies(i):
            c.start()
        return 0

    nm = x.shape[1] // 256
    lax.fori_loop(0, nm, d13_body, 0)

    def d2_copy(i):
        m = pl.ds(pl.multiple_of(i * 128, 128), 128)
        return pltpu.make_async_copy(acc2.at[m], o2.at[e, m], osem.at[2])

    def d2_body(i, _):
        m = pl.ds(pl.multiple_of(i * 128, 128), 128)
        acc(acc2, m, lax.dot_general(a[:, m], y[...], (((0,), (0,)), ((), ())), preferred_element_type=F32))
        d2_copy(i).start()
        return 0

    lax.fori_loop(0, fs // 128, d2_body, 0)

    def drain13(i, _):
        for c in out_copies(i):
            c.wait()
        return 0

    def drain2(i, _):
        d2_copy(i).wait()
        return 0

    lax.fori_loop(0, nm, drain13, 0)
    lax.fori_loop(0, fs // 128, drain2, 0)


def _dw_call(e, idx, xs, ys, w1, w3, w2, prev, first):
    el, d, f = w1.shape
    n, rows = len(xs), xs[0].shape[0]
    fs = f // 8
    anyspec = pl.BlockSpec(memory_space=pl.ANY)
    outs = [jax.ShapeDtypeStruct((el, d, fs), F32), jax.ShapeDtypeStruct((el, d, fs), F32),
            jax.ShapeDtypeStruct((el, fs, d), F32)]
    args = [idx, *xs, *ys, w1, w3, w2]
    alias = {}
    if prev is not None:
        alias = {len(args) + i: i for i in range(3)}
        args += list(prev)
    return pl.pallas_call(
        functools.partial(_dw_kernel, e, n, first),
        out_shape=outs,
        in_specs=[pl.BlockSpec(memory_space=pltpu.SMEM)] + [anyspec] * (len(args) - 1),
        out_specs=[anyspec] * 3,
        scratch_shapes=[
            pltpu.VMEM((n * rows, d), BF16),
            pltpu.VMEM((n * rows, d), BF16),
            pltpu.VMEM((d, 2 * fs), BF16),
            pltpu.VMEM((fs, d), BF16),
            pltpu.VMEM((n * rows, 2 * fs), BF16),
            pltpu.VMEM((n * rows, fs), BF16),
            pltpu.VMEM((d, 2 * fs), F32),
            pltpu.VMEM((fs, d), F32),
            pltpu.SemaphoreType.DMA((6,)),
            pltpu.SemaphoreType.DMA((n,)),
            pltpu.SemaphoreType.DMA((n,)),
            pltpu.SemaphoreType.DMA((3,)),
        ],
        input_output_aliases=alias,
        cost_estimate=pl.CostEstimate(flops=12 * n * rows * d * fs, bytes_accessed=n * 2 * 2**20 + 9 * 2**20,
                                      transcendentals=n * rows * fs),
    )(*args)


def solution(mesh):
    np_ = mesh.shape['expert']
    tok = P(('data', 'expert'), None)
    buf = P(('data', 'expert'), None, None)
    wsp = P('expert', None, None)

    def body(dy, gates, topk_idx, slot, yd, xd, h1, h3, w1, w3, w2):
        d = dy.shape[1]
        el = w1.shape[0]
        cap = xd.shape[1] // np_
        idx = lax.axis_index('data').astype(jnp.int32).reshape(1)

        used = (jnp.max(jnp.abs(xd.astype(F32)), axis=-1) > 0.0).astype(BF16)
        rows = xd.shape[1]
        at = lax.broadcasted_iota(jnp.int32, (rows, rows), 0)
        to = lax.broadcasted_iota(jnp.int32, (rows, rows), 1)
        rank = jnp.dot(used, (at < to).astype(BF16), preferred_element_type=F32)
        count = jnp.sum(used.astype(F32), axis=1)
        room = PACK - count[0]
        far = jnp.where(rank[1] < room, PACK - 1 - rank[1], PACK + rank[1] - room)
        pos = jnp.where(used > 0, jnp.stack([rank[0], far]), -1.0).reshape(1, el * rows)
        kept = jnp.stack([count[0], jnp.minimum(count[1], room)])
        eighth = jnp.floor(kept / 8.0)
        meta = jnp.stack([eighth, kept - 8.0 * eighth], axis=1).reshape(4)
        over = (count[0] + count[1] > PACK).astype(F32)
        halves = ((0, PACK // 2, True), (PACK // 2, PACK // 2, False))

        def chain(c, last_right):
            r, l = [c], [c]
            for _ in range(3):
                r.append([lax.ppermute(v, 'data', RIGHT) for v in r[-1]])
                l.append([lax.ppermute(v, 'data', LEFT) for v in l[-1]])
            perm, last = (RIGHT, r[3]) if last_right else (LEFT, l[3])
            r.append([lax.ppermute(v, 'data', perm) for v in last])
            return r, l

        xr, xl = chain(_pack(xd, pos, meta, halves, el, False), True)

        v = (gates[:, :, None] * dy.astype(F32)[:, None, :]).astype(BF16)
        blk = el * cap + META
        ex, sl = topk_idx[:, 0], slot[:, 0]
        row = jnp.where(sl >= 0, ex * cap + (ex // el) * META + sl, -1).reshape(1, -1)
        send = _send(row, over.reshape(1), v[:, 0], np_, blk)
        recv = lax.all_to_all(send.reshape(np_, blk, d), 'expert', 0, 0, tiled=True)
        dyd = jnp.swapaxes(recv[:, :el * cap].reshape(np_, el, cap, d), 0, 1).reshape(el, np_ * cap, d)
        yr, yl = chain(_pack(recv, pos, meta, halves, el, True), False)
        dg = jnp.einsum('tkd,td->tk', yd, dy, preferred_element_type=F32)

        h1f = h1.astype(F32)
        h3f = h3.astype(F32)
        s = jax.nn.sigmoid(h1f)
        silu = h1f * s
        da = jnp.einsum('ecd,efd->ecf', dyd, w2, preferred_element_type=F32).astype(BF16).astype(F32)
        dh1 = (da * h3f * s * (1.0 + h1f * (1.0 - s))).astype(BF16)
        dh3 = (da * silu).astype(BF16)
        dxd = (jnp.einsum('ecf,edf->ecd', dh1, w1, preferred_element_type=F32)
               + jnp.einsum('ecf,edf->ecd', dh3, w3, preferred_element_type=F32)).astype(BF16)
        out = jnp.swapaxes(dxd.reshape(el, np_, cap, d), 0, 1)
        back = lax.all_to_all(out, 'expert', 0, 0, tiled=True).reshape(np_ * el * cap, d)
        dx = _unpack(jnp.where(sl >= 0, ex * cap + sl, -1)[:, None], back)

        acc = None
        for pick in (lambda r, l: (r[0], r[1], l[1]), lambda r, l: (r[2], l[2]),
                     lambda r, l: (r[3], l[3]), lambda r, l: (r[4],)):
            acc = _dwp_call(idx, pick(xr, xl), pick(yr, yl), w1, w3, w2, acc)

        acc, some = acc[:3], acc[3][0, 0] > 0
        rest = ((PACK, el * rows - PACK, False),)

        def spill(acc):
            xo, = _pack(xd, pos, meta, rest, el, False)
            yo, = _pack(recv, pos, meta, rest, el, True)

            def hop(_, st):
                xo, yo, acc = st
                acc = _dw_call(1, idx, [xo], [yo], w1, w3, w2, acc, False)
                return lax.ppermute(xo, 'data', RIGHT), lax.ppermute(yo, 'data', RIGHT), tuple(acc)

            return lax.fori_loop(0, 8, hop, (xo, yo, acc))[2]

        acc = lax.cond(some, spill, lambda acc: acc, tuple(acc))
        dw1, dw3, dw2 = acc
        return dx, dg, dw1, dw3, dw2

    return jax.shard_map(body, mesh=mesh,
                         in_specs=(tok, tok, tok, tok, buf, buf, buf, buf, wsp, wsp, wsp),
                         out_specs=(tok, tok, P('expert', None, 'data'), P('expert', None, 'data'), P('expert', 'data', None)),
                         check_vma=False)
```

```python
import functools

import jax
import jax.numpy as jnp
from jax import lax
from jax.experimental import pallas as pl
from jax.experimental.pallas import tpu as pltpu
from jax.sharding import PartitionSpec as P


F32 = jnp.float32
BF16 = jnp.bfloat16


PACK = 1088
META = 16
TILE = 256
FRONT = 576
RING = (0, 2, 4, 6, 7, 5, 3, 1)
RIGHT = [(RING[i], RING[(i + 1) % 8]) for i in range(8)]
LEFT = [(RING[(i + 1) % 8], RING[i]) for i in range(8)]


def _pack_kernel(grouped, el, starts, pos_ref, meta_ref, src_ref, *refs):
    n = len(starts)
    outs, src, fl, sem = refs[:n], refs[n], refs[n + 1], refs[n + 2]
    cps = []
    if grouped:
        np_ = src_ref.shape[0]
        cap = (src_ref.shape[1] - META) // el
        for p in range(np_):
            for e in range(el):
                dst = src.at[pl.ds(e * np_ * cap + p * cap, cap)]
                cps.append(pltpu.make_async_copy(src_ref.at[p, pl.ds(e * cap, cap)], dst, sem.at[p * el + e]))
            cps.append(pltpu.make_async_copy(src_ref.at[p, pl.ds(el * cap, META)], fl.at[pl.ds(p * META, META)],
                                             sem.at[np_ * el + p]))
    else:
        rows = src_ref.shape[1]
        for e in range(el):
            cps.append(pltpu.make_async_copy(src_ref.at[e], src.at[pl.ds(e * rows, rows)], sem.at[e]))
    for c in cps:
        c.start()
    for c in cps:
        c.wait()
    pos = pos_ref[...]
    for o, (base, rows, meta) in zip(outs, starts):
        def tile_body(i, _, o=o, base=base):
            r = pl.multiple_of(i * 64, 64)
            row = (lax.broadcasted_iota(jnp.int32, (64, 1), 0) + (r + base)).astype(F32)
            hot = jnp.where(pos == row, 1.0, 0.0).astype(BF16)
            o[pl.ds(r, 64), :] = jnp.dot(hot, src[...], preferred_element_type=F32).astype(BF16)
            return 0

        lax.fori_loop(0, rows // 64, tile_body, 0)
        if meta and grouped:
            v = fl[pl.ds(0, META), :].astype(F32)
            for p in range(1, np_):
                v = jnp.maximum(v, fl[pl.ds(p * META, META), :].astype(F32))
            o[pl.ds(rows, META), :] = v.astype(BF16)
        elif meta:
            k = lax.broadcasted_iota(jnp.int32, (META, o.shape[1]), 0)
            v = jnp.where(k == 0, meta_ref[0], jnp.where(k == 1, meta_ref[1], jnp.where(k == 2, meta_ref[2], meta_ref[3])))
            o[pl.ds(rows, META), :] = v.astype(BF16)


def _pack(src, pos, meta, starts, el, grouped):
    d = src.shape[-1]
    rows = pos.shape[1]
    vspec = pl.BlockSpec(memory_space=pltpu.VMEM)
    total = sum(r for _, r, _ in starts)
    return pl.pallas_call(
        functools.partial(_pack_kernel, grouped, el, starts),
        out_shape=[jax.ShapeDtypeStruct((r + META * m, d), BF16) for _, r, m in starts],
        in_specs=[vspec, pl.BlockSpec(memory_space=pltpu.SMEM), pl.BlockSpec(memory_space=pl.ANY)],
        out_specs=[vspec] * len(starts),
        scratch_shapes=[pltpu.VMEM((rows, d), BF16), pltpu.VMEM((4 * META, d), BF16), pltpu.SemaphoreType.DMA((12,))],
        cost_estimate=pl.CostEstimate(flops=2 * total * rows * d, bytes_accessed=2 * (rows + total) * d, transcendentals=0),
    )(pos, meta, src)


def _send_kernel(blk, over_ref, to_ref, v_ref, o_ref):
    rows = o_ref.shape[0] // 8

    def tile_body(i, _):
        r = pl.multiple_of(i * rows, 8)
        line = lax.broadcasted_iota(jnp.int32, (rows, v_ref.shape[0]), 0) + r
        hot = jnp.where(to_ref[...] == line, 1.0, 0.0).astype(BF16)
        o_ref[pl.ds(r, rows), :] = jnp.dot(hot, v_ref[...], preferred_element_type=F32).astype(BF16)
        return 0

    lax.fori_loop(0, 8, tile_body, 0)
    for b in range(o_ref.shape[0] // blk):
        o_ref[pl.ds((b + 1) * blk - META, META), :] = jnp.full((META, o_ref.shape[1]), over_ref[0], F32).astype(BF16)


def _send(to, over, v, np_, blk):
    t, d = v.shape
    vspec = pl.BlockSpec(memory_space=pltpu.VMEM)
    return pl.pallas_call(
        functools.partial(_send_kernel, blk),
        out_shape=jax.ShapeDtypeStruct((np_ * blk, d), BF16),
        in_specs=[pl.BlockSpec(memory_space=pltpu.SMEM), vspec, vspec],
        out_specs=vspec,
        cost_estimate=pl.CostEstimate(flops=2 * t * np_ * blk * d, bytes_accessed=2 * (t + np_ * blk) * d, transcendentals=0),
        name="send",
    )(over, to, v)


def _unpack_kernel(at_ref, src_ref, o_ref):
    def tile_body(i, _):
        r = pl.ds(pl.multiple_of(i * 128, 128), 128)
        lane = lax.broadcasted_iota(jnp.int32, (128, src_ref.shape[0]), 1)
        hot = jnp.where(at_ref[r, :] == lane, 1.0, 0.0).astype(BF16)
        o_ref[r, :] = jnp.dot(hot, src_ref[...], preferred_element_type=F32).astype(BF16)
        return 0

    lax.fori_loop(0, o_ref.shape[0] // 128, tile_body, 0)


def _unpack(at, src):
    t, (rows, d) = at.shape[0], src.shape
    vspec = pl.BlockSpec(memory_space=pltpu.VMEM)
    return pl.pallas_call(
        _unpack_kernel,
        out_shape=jax.ShapeDtypeStruct((t, d), BF16),
        in_specs=[vspec, vspec],
        out_specs=vspec,
        cost_estimate=pl.CostEstimate(flops=2 * t * rows * d, bytes_accessed=2 * (rows + t) * d, transcendentals=0),
        name="unpack",
    )(at, src)


def _dwp_kernel(n, first, idx_ref, *refs):
    xc, yc = refs[:2 * n], refs[2 * n:4 * n]
    w1, w3, w2 = refs[4 * n:4 * n + 3]
    o1, o3, o2, oflag = refs[-19:-15]
    x, y, xm, ym, w13, w2s, dh, a, acc13, acc2, wsem, xsem, ysem, msem, osem = refs[-15:]
    el, fs, d = w2s.shape
    hp = FRONT
    f0 = pl.multiple_of(idx_ref[0] * fs, 128)
    half = lambda j: pl.ds(j * fs, fs)

    def w_copies(e):
        return [pltpu.make_async_copy(w1.at[e, :, pl.ds(f0, fs)], w13.at[e, :, half(0)], wsem.at[0, e]),
                pltpu.make_async_copy(w3.at[e, :, pl.ds(f0, fs)], w13.at[e, :, half(1)], wsem.at[1, e]),
                pltpu.make_async_copy(w2.at[e, pl.ds(f0, fs), :], w2s.at[e], wsem.at[2, e])]

    def prev_copies(e):
        return [pltpu.make_async_copy(o1.at[e], acc13.at[e, :, half(0)], wsem.at[3, e]),
                pltpu.make_async_copy(o3.at[e], acc13.at[e, :, half(1)], wsem.at[4, e]),
                pltpu.make_async_copy(o2.at[e], acc2.at[e], wsem.at[5, e])]

    def row_copies(s, xp, yp):
        at = lambda k: pl.ds(pl.multiple_of(s * PACK + k * hp, 64), (hp, PACK - hp)[k])
        mt = pl.ds(pl.multiple_of(s * META, META), META)
        return [pltpu.make_async_copy(xp[0].at[pl.ds(hp, META)], xm.at[mt], msem.at[0, s]),
                pltpu.make_async_copy(yp[0].at[pl.ds(hp, META)], ym.at[mt], msem.at[1, s]),
                pltpu.make_async_copy(xp[0].at[pl.ds(0, hp)], x.at[at(0)], xsem.at[0, s]),
                pltpu.make_async_copy(yp[0].at[pl.ds(0, hp)], y.at[at(0)], ysem.at[0, s]),
                pltpu.make_async_copy(xp[1], x.at[at(1)], xsem.at[1, s]),
                pltpu.make_async_copy(yp[1], y.at[at(1)], ysem.at[1, s])]

    def out_copies(e):
        return [pltpu.make_async_copy(acc13.at[e, :, half(0)], o1.at[e], osem.at[0, e]),
                pltpu.make_async_copy(acc13.at[e, :, half(1)], o3.at[e], osem.at[1, e]),
                pltpu.make_async_copy(acc2.at[e], o2.at[e], osem.at[2, e])]

    for c in w_copies(0):
        c.start()
    for s in range(n):
        for c in row_copies(s, xc[2 * s:2 * s + 2], yc[2 * s:2 * s + 2]):
            c.start()
        if s == 0 and not first:
            for c in prev_copies(0):
                c.start()
    for c in w_copies(1):
        c.start()
    if first:
        acc13[...] = jnp.zeros_like(acc13)
        acc2[...] = jnp.zeros_like(acc2)
    else:
        for c in prev_copies(1):
            c.start()

    def expert_body(e, _):
        sign = (1 - 2 * e).astype(F32)
        for c in w_copies(e):
            c.wait()
        if not first:
            for c in prev_copies(e):
                c.wait()

        def group_body(s, _):
            @pl.when(e == 0)
            def _():
                for c in row_copies(s, xc[:2], yc[:2]):
                    c.wait()

            m = xm[pl.ds(pl.multiple_of(s * META, META), META), :128].astype(F32)
            cut = jnp.max(m[0:1, :] * 8.0 + m[1:2, :])
            other = jnp.max(m[2:3, :] * 8.0 + m[3:4, :])
            used = jnp.where(e == 0, cut, other).astype(jnp.int32)

            def tile_body(k, _):
                base = jnp.where(e == 0, k * TILE, PACK - TILE - k * TILE)
                r = pl.ds(pl.multiple_of(s * PACK + base, 64), TILE)
                row = (lax.broadcasted_iota(jnp.int32, (TILE, fs), 0) + base).astype(F32)
                keep = (cut - row - 0.5) * sign > 0.0
                h = jnp.dot(x[r, :], w13[e], preferred_element_type=F32).astype(BF16).astype(F32)
                da = lax.dot_general(y[r, :], w2s[e], (((1,), (1,)), ((), ())),
                                     preferred_element_type=F32).astype(BF16).astype(F32)
                h1 = jnp.where(keep, h[:, :fs], 0.0)
                h3 = jnp.where(keep, h[:, fs:], 0.0)
                da = jnp.where(keep, da, 0.0)
                sg = jax.nn.sigmoid(h1)
                silu = h1 * sg
                a[...] = (silu * h3).astype(BF16)
                dh[:, :fs] = (da * h3 * sg * (1.0 + h1 * (1.0 - sg))).astype(BF16)
                dh[:, fs:] = (da * silu).astype(BF16)
                for i in range(d // 256):
                    m = slice(i * 256, (i + 1) * 256)
                    acc13[e, m, :] += lax.dot_general(x[r, m], dh[...], (((0,), (0,)), ((), ())), preferred_element_type=F32)
                acc2[e] += lax.dot_general(a[...], y[r, :], (((0,), (0,)), ((), ())), preferred_element_type=F32)
                return 0

            lax.fori_loop(0, (used + (TILE - 1)) // TILE, tile_body, 0)
            return 0

        lax.fori_loop(0, n, group_body, 0)
        for c in out_copies(e):
            c.start()
        return 0

    lax.fori_loop(0, el, expert_body, 0)
    flag = ym[pl.ds(0, META), :].astype(F32)
    for s in range(1, n):
        flag = jnp.maximum(flag, ym[pl.ds(s * META, META), :].astype(F32))
    if not first:
        flag = jnp.maximum(flag, refs[4 * n + 6][...])
    oflag[...] = flag
    for e in range(el):
        for c in out_copies(e):
            c.wait()


def _dwp_call(idx, xs, ys, w1, w3, w2, prev):
    el, d, f = w1.shape
    n = len(xs)
    fs = f // 8
    anyspec = pl.BlockSpec(memory_space=pl.ANY)
    vspec = pl.BlockSpec(memory_space=pltpu.VMEM)
    outs = [jax.ShapeDtypeStruct((el, d, fs), F32), jax.ShapeDtypeStruct((el, d, fs), F32),
            jax.ShapeDtypeStruct((el, fs, d), F32), jax.ShapeDtypeStruct((META, d), F32)]
    args = [idx, *(c for p in xs for c in p), *(c for p in ys for c in p), w1, w3, w2]
    specs = [pl.BlockSpec(memory_space=pltpu.SMEM)] + [anyspec] * (len(args) - 1)
    alias = {}
    if prev is not None:
        alias = {len(args) + i: i for i in range(3)}
        args += list(prev)
        specs += [anyspec] * 3 + [vspec]
    return pl.pallas_call(
        functools.partial(_dwp_kernel, n, prev is None),
        out_shape=outs,
        in_specs=specs,
        out_specs=[anyspec] * 3 + [vspec],
        scratch_shapes=[
            pltpu.VMEM((n * PACK, d), BF16),
            pltpu.VMEM((n * PACK, d), BF16),
            pltpu.VMEM((n * META, d), BF16),
            pltpu.VMEM((n * META, d), BF16),
            pltpu.VMEM((el, d, 2 * fs), BF16),
            pltpu.VMEM((el, fs, d), BF16),
            pltpu.VMEM((TILE, 2 * fs), BF16),
            pltpu.VMEM((TILE, fs), BF16),
            pltpu.VMEM((el, d, 2 * fs), F32),
            pltpu.VMEM((el, fs, d), F32),
            pltpu.SemaphoreType.DMA((6, el)),
            pltpu.SemaphoreType.DMA((2, n)),
            pltpu.SemaphoreType.DMA((2, n)),
            pltpu.SemaphoreType.DMA((2, n)),
            pltpu.SemaphoreType.DMA((3, el)),
        ],
        input_output_aliases=alias,
        cost_estimate=pl.CostEstimate(flops=12 * n * PACK * d * fs, bytes_accessed=n * 4 * 2**20 + 18 * 2**20,
                                      transcendentals=n * PACK * fs),
    )(*args)


def _dw_kernel(e, n, first, idx_ref, *refs):
    xs, ys = refs[:n], refs[n:2 * n]
    w1, w3, w2 = refs[2 * n:2 * n + 3]
    o1, o3, o2 = refs[-15:-12]
    x, y, w13, w2s, dh, a, acc13, acc2, wsem, xsem, ysem, osem = refs[-12:]
    rows = xs[0].shape[0]
    fs = w2s.shape[0]
    tile = 64
    per = rows // tile
    f0 = pl.multiple_of(idx_ref[0] * fs, 128)
    half = lambda j: pl.ds(j * fs, fs)

    def row_copy(src, dst, j, sem):
        return pltpu.make_async_copy(src, dst.at[pl.ds(pl.multiple_of(j * rows, 64), rows)], sem.at[j])

    wcp = [
        pltpu.make_async_copy(w1.at[e, :, pl.ds(f0, fs)], w13.at[:, half(0)], wsem.at[0]),
        pltpu.make_async_copy(w3.at[e, :, pl.ds(f0, fs)], w13.at[:, half(1)], wsem.at[1]),
        pltpu.make_async_copy(w2.at[e, pl.ds(f0, fs), :], w2s, wsem.at[2]),
    ]
    row_copy(xs[0], x, 0, xsem).start()
    for c in wcp:
        c.start()
    row_copy(ys[0], y, 0, ysem).start()
    for j in range(1, n):
        row_copy(xs[j], x, j, xsem).start()
        row_copy(ys[j], y, j, ysem).start()
    prev = []
    if not first:
        prev = [
            pltpu.make_async_copy(o1.at[e], acc13.at[:, half(0)], wsem.at[3]),
            pltpu.make_async_copy(o3.at[e], acc13.at[:, half(1)], wsem.at[4]),
            pltpu.make_async_copy(o2.at[e], acc2, wsem.at[5]),
        ]
        for c in prev:
            c.start()
    for c in wcp:
        c.wait()

    def rows_body(i, _):
        @pl.when(lax.rem(i, per) == 0)
        def _():
            row_copy(xs[0], x, i // per, xsem).wait()
            row_copy(ys[0], y, i // per, ysem).wait()

        r = pl.ds(pl.multiple_of(i * tile, 64), tile)
        h = jnp.dot(x[r, :], w13[...], preferred_element_type=F32).astype(BF16).astype(F32)
        da = lax.dot_general(y[r, :], w2s[...], (((1,), (1,)), ((), ())),
                             preferred_element_type=F32).astype(BF16).astype(F32)
        h1, h3 = h[:, :fs], h[:, fs:]
        s = jax.nn.sigmoid(h1)
        silu = h1 * s
        a[r, :] = (silu * h3).astype(BF16)
        dh[r, :fs] = (da * h3 * s * (1.0 + h1 * (1.0 - s))).astype(BF16)
        dh[r, fs:] = (da * silu).astype(BF16)
        return 0

    lax.fori_loop(0, per * n, rows_body, 0)
    for c in prev:
        c.wait()

    def acc(ref, m, val):
        if first:
            ref[m, :] = val
        else:
            ref[m, :] += val

    def out_copies(i):
        m = pl.ds(pl.multiple_of(i * 256, 256), 256)
        return (pltpu.make_async_copy(acc13.at[m, half(0)], o1.at[e, m], osem.at[0]),
                pltpu.make_async_copy(acc13.at[m, half(1)], o3.at[e, m], osem.at[1]))

    def d13_body(i, _):
        m = pl.ds(pl.multiple_of(i * 256, 256), 256)
        acc(acc13, m, lax.dot_general(x[:, m], dh[...], (((0,), (0,)), ((), ())), preferred_element_type=F32))
        for c in out_copies(i):
            c.start()
        return 0

    nm = x.shape[1] // 256
    lax.fori_loop(0, nm, d13_body, 0)

    def d2_copy(i):
        m = pl.ds(pl.multiple_of(i * 128, 128), 128)
        return pltpu.make_async_copy(acc2.at[m], o2.at[e, m], osem.at[2])

    def d2_body(i, _):
        m = pl.ds(pl.multiple_of(i * 128, 128), 128)
        acc(acc2, m, lax.dot_general(a[:, m], y[...], (((0,), (0,)), ((), ())), preferred_element_type=F32))
        d2_copy(i).start()
        return 0

    lax.fori_loop(0, fs // 128, d2_body, 0)

    def drain13(i, _):
        for c in out_copies(i):
            c.wait()
        return 0

    def drain2(i, _):
        d2_copy(i).wait()
        return 0

    lax.fori_loop(0, nm, drain13, 0)
    lax.fori_loop(0, fs // 128, drain2, 0)


def _dw_call(e, idx, xs, ys, w1, w3, w2, prev, first):
    el, d, f = w1.shape
    n, rows = len(xs), xs[0].shape[0]
    fs = f // 8
    anyspec = pl.BlockSpec(memory_space=pl.ANY)
    outs = [jax.ShapeDtypeStruct((el, d, fs), F32), jax.ShapeDtypeStruct((el, d, fs), F32),
            jax.ShapeDtypeStruct((el, fs, d), F32)]
    args = [idx, *xs, *ys, w1, w3, w2]
    alias = {}
    if prev is not None:
        alias = {len(args) + i: i for i in range(3)}
        args += list(prev)
    return pl.pallas_call(
        functools.partial(_dw_kernel, e, n, first),
        out_shape=outs,
        in_specs=[pl.BlockSpec(memory_space=pltpu.SMEM)] + [anyspec] * (len(args) - 1),
        out_specs=[anyspec] * 3,
        scratch_shapes=[
            pltpu.VMEM((n * rows, d), BF16),
            pltpu.VMEM((n * rows, d), BF16),
            pltpu.VMEM((d, 2 * fs), BF16),
            pltpu.VMEM((fs, d), BF16),
            pltpu.VMEM((n * rows, 2 * fs), BF16),
            pltpu.VMEM((n * rows, fs), BF16),
            pltpu.VMEM((d, 2 * fs), F32),
            pltpu.VMEM((fs, d), F32),
            pltpu.SemaphoreType.DMA((6,)),
            pltpu.SemaphoreType.DMA((n,)),
            pltpu.SemaphoreType.DMA((n,)),
            pltpu.SemaphoreType.DMA((3,)),
        ],
        input_output_aliases=alias,
        cost_estimate=pl.CostEstimate(flops=12 * n * rows * d * fs, bytes_accessed=n * 2 * 2**20 + 9 * 2**20,
                                      transcendentals=n * rows * fs),
    )(*args)


def solution(mesh):
    np_ = mesh.shape['expert']
    tok = P(('data', 'expert'), None)
    buf = P(('data', 'expert'), None, None)
    wsp = P('expert', None, None)

    def body(dy, gates, topk_idx, slot, yd, xd, h1, h3, w1, w3, w2):
        d = dy.shape[1]
        el = w1.shape[0]
        cap = xd.shape[1] // np_
        idx = lax.axis_index('data').astype(jnp.int32).reshape(1)

        used = (jnp.max(jnp.abs(xd.astype(F32)), axis=-1) > 0.0).astype(BF16)
        rows = xd.shape[1]
        at = lax.broadcasted_iota(jnp.int32, (rows, rows), 0)
        to = lax.broadcasted_iota(jnp.int32, (rows, rows), 1)
        rank = jnp.dot(used, (at < to).astype(BF16), preferred_element_type=F32)
        count = jnp.sum(used.astype(F32), axis=1)
        room = PACK - count[0]
        far = jnp.where(rank[1] < room, PACK - 1 - rank[1], PACK + rank[1] - room)
        pos = jnp.where(used > 0, jnp.stack([rank[0], far]), -1.0).reshape(1, el * rows)
        kept = jnp.stack([count[0], jnp.minimum(count[1], room)])
        eighth = jnp.floor(kept / 8.0)
        meta = jnp.stack([eighth, kept - 8.0 * eighth], axis=1).reshape(4)
        over = (count[0] + count[1] > PACK).astype(F32)
        halves = ((0, FRONT, True), (FRONT, PACK - FRONT, False))

        def chain(c, last_right):
            r, l = [c], [c]
            for _ in range(3):
                r.append([lax.ppermute(v, 'data', RIGHT) for v in r[-1]])
                l.append([lax.ppermute(v, 'data', LEFT) for v in l[-1]])
            perm, last = (RIGHT, r[3]) if last_right else (LEFT, l[3])
            r.append([lax.ppermute(v, 'data', perm) for v in last])
            return r, l

        xr, xl = chain(_pack(xd, pos, meta, halves, el, False), True)

        v = (gates[:, :, None] * dy.astype(F32)[:, None, :]).astype(BF16)
        blk = el * cap + META
        ex, sl = topk_idx[:, 0], slot[:, 0]
        row = jnp.where(sl >= 0, ex * cap + (ex // el) * META + sl, -1).reshape(1, -1)
        send = _send(row, over.reshape(1), v[:, 0], np_, blk)
        recv = lax.all_to_all(send.reshape(np_, blk, d), 'expert', 0, 0, tiled=True)
        dyd = jnp.swapaxes(recv[:, :el * cap].reshape(np_, el, cap, d), 0, 1).reshape(el, np_ * cap, d)
        yr, yl = chain(_pack(recv, pos, meta, halves, el, True), False)
        dg = jnp.einsum('tkd,td->tk', yd, dy, preferred_element_type=F32)

        h1f = h1.astype(F32)
        h3f = h3.astype(F32)
        s = jax.nn.sigmoid(h1f)
        silu = h1f * s
        da = jnp.einsum('ecd,efd->ecf', dyd, w2, preferred_element_type=F32).astype(BF16).astype(F32)
        dh1 = (da * h3f * s * (1.0 + h1f * (1.0 - s))).astype(BF16)
        dh3 = (da * silu).astype(BF16)
        dxd = (jnp.einsum('ecf,edf->ecd', dh1, w1, preferred_element_type=F32)
               + jnp.einsum('ecf,edf->ecd', dh3, w3, preferred_element_type=F32)).astype(BF16)
        out = jnp.swapaxes(dxd.reshape(el, np_, cap, d), 0, 1)
        back = lax.all_to_all(out, 'expert', 0, 0, tiled=True).reshape(np_ * el * cap, d)
        dx = _unpack(jnp.where(sl >= 0, ex * cap + sl, -1)[:, None], back)

        acc = None
        for pick in (lambda r, l: (r[0], r[1], l[1]), lambda r, l: (r[2], l[2]),
                           lambda r, l: (r[3], l[3]), lambda r, l: (r[4],)):
            acc = _dwp_call(idx, pick(xr, xl), pick(yr, yl), w1, w3, w2, acc)

        acc, some = acc[:3], acc[3][0, 0] > 0
        rest = ((PACK, el * rows - PACK, False),)

        def spill(acc):
            xo, = _pack(xd, pos, meta, rest, el, False)
            yo, = _pack(recv, pos, meta, rest, el, True)

            acc = _dw_call(1, idx, [xo], [yo], w1, w3, w2, acc, False)

            def hop(_, st):
                xa, ya, xb, yb, acc = st
                xa, ya = (lax.ppermute(c, 'data', RIGHT) for c in (xa, ya))
                xb, yb = (lax.ppermute(c, 'data', LEFT) for c in (xb, yb))
                return xa, ya, xb, yb, tuple(_dw_call(1, idx, [xa, xb], [ya, yb], w1, w3, w2, acc, False))

            xa, ya, _, _, acc = lax.fori_loop(0, 3, hop, (xo, yo, xo, yo, tuple(acc)))
            xa, ya = (lax.ppermute(c, 'data', RIGHT) for c in (xa, ya))
            return tuple(_dw_call(1, idx, [xa], [ya], w1, w3, w2, acc, False))

        acc = lax.cond(some, spill, lambda acc: acc, tuple(acc))
        dw1, dw3, dw2 = acc
        return dx, dg, dw1, dw3, dw2

    return jax.shard_map(body, mesh=mesh,
                         in_specs=(tok, tok, tok, tok, buf, buf, buf, buf, wsp, wsp, wsp),
                         out_specs=(tok, tok, P('expert', None, 'data'), P('expert', None, 'data'), P('expert', 'data', None)),
                         check_vma=False)
```

```python
import functools

import jax
import jax.numpy as jnp
from jax import lax
from jax.experimental import pallas as pl
from jax.experimental.pallas import tpu as pltpu
from jax.sharding import PartitionSpec as P


F32 = jnp.float32
BF16 = jnp.bfloat16


PACK = 1088
META = 16
TILE = 256
FRONT = 544
RING = (0, 2, 4, 6, 7, 5, 3, 1)
RIGHT = [(RING[i], RING[(i + 1) % 8]) for i in range(8)]
LEFT = [(RING[(i + 1) % 8], RING[i]) for i in range(8)]


def _pack_kernel(grouped, el, starts, pos_ref, meta_ref, src_ref, *refs):
    n = len(starts)
    outs, src, fl, sem = refs[:n], refs[n], refs[n + 1], refs[n + 2]
    cps = []
    if grouped:
        np_ = src_ref.shape[0]
        cap = (src_ref.shape[1] - META) // el
        for p in range(np_):
            for e in range(el):
                dst = src.at[pl.ds(e * np_ * cap + p * cap, cap)]
                cps.append(pltpu.make_async_copy(src_ref.at[p, pl.ds(e * cap, cap)], dst, sem.at[p * el + e]))
            cps.append(pltpu.make_async_copy(src_ref.at[p, pl.ds(el * cap, META)], fl.at[pl.ds(p * META, META)],
                                             sem.at[np_ * el + p]))
    else:
        rows = src_ref.shape[1]
        for e in range(el):
            cps.append(pltpu.make_async_copy(src_ref.at[e], src.at[pl.ds(e * rows, rows)], sem.at[e]))
    for c in cps:
        c.start()
    for c in cps:
        c.wait()
    pos = pos_ref[...]
    for o, (base, rows, meta) in zip(outs, starts):
        tile = rows // 2

        def tile_body(i, _, o=o, base=base, tile=tile):
            r = pl.multiple_of(i * tile, 16)
            row = (lax.broadcasted_iota(jnp.int32, (tile, 1), 0) + (r + base)).astype(F32)
            hot = jnp.where(pos == row, 1.0, 0.0).astype(BF16)
            o[pl.ds(r, tile), :] = jnp.dot(hot, src[...], preferred_element_type=F32).astype(BF16)
            return 0

        lax.fori_loop(0, 2, tile_body, 0)
        if meta and grouped:
            v = fl[pl.ds(0, META), :].astype(F32)
            for p in range(1, np_):
                v = jnp.maximum(v, fl[pl.ds(p * META, META), :].astype(F32))
            o[pl.ds(rows, META), :] = v.astype(BF16)
        elif meta:
            k = lax.broadcasted_iota(jnp.int32, (META, o.shape[1]), 0)
            v = jnp.where(k == 0, meta_ref[0], jnp.where(k == 1, meta_ref[1], jnp.where(k == 2, meta_ref[2], meta_ref[3])))
            o[pl.ds(rows, META), :] = v.astype(BF16)


def _pack(src, pos, meta, starts, el, grouped):
    d = src.shape[-1]
    rows = pos.shape[1]
    vspec = pl.BlockSpec(memory_space=pltpu.VMEM)
    total = sum(r for _, r, _ in starts)
    return pl.pallas_call(
        functools.partial(_pack_kernel, grouped, el, starts),
        out_shape=[jax.ShapeDtypeStruct((r + META * m, d), BF16) for _, r, m in starts],
        in_specs=[vspec, pl.BlockSpec(memory_space=pltpu.SMEM), pl.BlockSpec(memory_space=pl.ANY)],
        out_specs=[vspec] * len(starts),
        scratch_shapes=[pltpu.VMEM((rows, d), BF16), pltpu.VMEM((4 * META, d), BF16), pltpu.SemaphoreType.DMA((12,))],
        cost_estimate=pl.CostEstimate(flops=2 * total * rows * d, bytes_accessed=2 * (rows + total) * d, transcendentals=0),
    )(pos, meta, src)


def _send_kernel(blk, over_ref, to_ref, v_ref, o_ref):
    rows = o_ref.shape[0] // 8

    def tile_body(i, _):
        r = pl.multiple_of(i * rows, 8)
        line = lax.broadcasted_iota(jnp.int32, (rows, v_ref.shape[0]), 0) + r
        hot = jnp.where(to_ref[...] == line, 1.0, 0.0).astype(BF16)
        o_ref[pl.ds(r, rows), :] = jnp.dot(hot, v_ref[...], preferred_element_type=F32).astype(BF16)
        return 0

    lax.fori_loop(0, 8, tile_body, 0)
    for b in range(o_ref.shape[0] // blk):
        o_ref[pl.ds((b + 1) * blk - META, META), :] = jnp.full((META, o_ref.shape[1]), over_ref[0], F32).astype(BF16)


def _send(to, over, v, np_, blk):
    t, d = v.shape
    vspec = pl.BlockSpec(memory_space=pltpu.VMEM)
    return pl.pallas_call(
        functools.partial(_send_kernel, blk),
        out_shape=jax.ShapeDtypeStruct((np_ * blk, d), BF16),
        in_specs=[pl.BlockSpec(memory_space=pltpu.SMEM), vspec, vspec],
        out_specs=vspec,
        cost_estimate=pl.CostEstimate(flops=2 * t * np_ * blk * d, bytes_accessed=2 * (t + np_ * blk) * d, transcendentals=0),
        name="send",
    )(over, to, v)


def _unpack_kernel(at_ref, src_ref, o_ref):
    def tile_body(i, _):
        r = pl.ds(pl.multiple_of(i * 128, 128), 128)
        lane = lax.broadcasted_iota(jnp.int32, (128, src_ref.shape[0]), 1)
        hot = jnp.where(at_ref[r, :] == lane, 1.0, 0.0).astype(BF16)
        o_ref[r, :] = jnp.dot(hot, src_ref[...], preferred_element_type=F32).astype(BF16)
        return 0

    lax.fori_loop(0, o_ref.shape[0] // 128, tile_body, 0)


def _unpack(at, src):
    t, (rows, d) = at.shape[0], src.shape
    vspec = pl.BlockSpec(memory_space=pltpu.VMEM)
    return pl.pallas_call(
        _unpack_kernel,
        out_shape=jax.ShapeDtypeStruct((t, d), BF16),
        in_specs=[vspec, vspec],
        out_specs=vspec,
        cost_estimate=pl.CostEstimate(flops=2 * t * rows * d, bytes_accessed=2 * (rows + t) * d, transcendentals=0),
        name="unpack",
    )(at, src)


def _dwp_kernel(n, first, idx_ref, *refs):
    xc, yc = refs[:2 * n], refs[2 * n:4 * n]
    w1, w3, w2 = refs[4 * n:4 * n + 3]
    o1, o3, o2, oflag = refs[-19:-15]
    x, y, xm, ym, w13, w2s, dh, a, acc13, acc2, wsem, xsem, ysem, msem, osem = refs[-15:]
    el, fs, d = w2s.shape
    hp = FRONT
    f0 = pl.multiple_of(idx_ref[0] * fs, 128)
    half = lambda j: pl.ds(j * fs, fs)

    def w_copies(e):
        return [pltpu.make_async_copy(w1.at[e, :, pl.ds(f0, fs)], w13.at[e, :, half(0)], wsem.at[0, e]),
                pltpu.make_async_copy(w3.at[e, :, pl.ds(f0, fs)], w13.at[e, :, half(1)], wsem.at[1, e]),
                pltpu.make_async_copy(w2.at[e, pl.ds(f0, fs), :], w2s.at[e], wsem.at[2, e])]

    def prev_copies(e):
        return [pltpu.make_async_copy(o1.at[e], acc13.at[e, :, half(0)], wsem.at[3, e]),
                pltpu.make_async_copy(o3.at[e], acc13.at[e, :, half(1)], wsem.at[4, e]),
                pltpu.make_async_copy(o2.at[e], acc2.at[e], wsem.at[5, e])]

    def row_copies(s, xp, yp):
        at = lambda k: pl.ds(pl.multiple_of(s * PACK + k * hp, 32), (hp, PACK - hp)[k])
        mt = pl.ds(pl.multiple_of(s * META, META), META)
        return [pltpu.make_async_copy(xp[0].at[pl.ds(hp, META)], xm.at[mt], msem.at[0, s]),
                pltpu.make_async_copy(yp[0].at[pl.ds(hp, META)], ym.at[mt], msem.at[1, s]),
                pltpu.make_async_copy(xp[0].at[pl.ds(0, hp)], x.at[at(0)], xsem.at[0, s]),
                pltpu.make_async_copy(yp[0].at[pl.ds(0, hp)], y.at[at(0)], ysem.at[0, s]),
                pltpu.make_async_copy(xp[1], x.at[at(1)], xsem.at[1, s]),
                pltpu.make_async_copy(yp[1], y.at[at(1)], ysem.at[1, s])]

    def out_copies(e):
        return [pltpu.make_async_copy(acc13.at[e, :, half(0)], o1.at[e], osem.at[0, e]),
                pltpu.make_async_copy(acc13.at[e, :, half(1)], o3.at[e], osem.at[1, e]),
                pltpu.make_async_copy(acc2.at[e], o2.at[e], osem.at[2, e])]

    for c in w_copies(0):
        c.start()
    for s in range(n):
        for c in row_copies(s, xc[2 * s:2 * s + 2], yc[2 * s:2 * s + 2]):
            c.start()
        if s == 0 and not first:
            for c in prev_copies(0):
                c.start()
    for c in w_copies(1):
        c.start()
    if first:
        acc13[...] = jnp.zeros_like(acc13)
        acc2[...] = jnp.zeros_like(acc2)
    else:
        for c in prev_copies(1):
            c.start()

    def expert_body(e, _):
        sign = (1 - 2 * e).astype(F32)
        for c in w_copies(e):
            c.wait()
        if not first:
            for c in prev_copies(e):
                c.wait()

        def group_body(s, _):
            @pl.when(e == 0)
            def _():
                for c in row_copies(s, xc[:2], yc[:2]):
                    c.wait()

            m = xm[pl.ds(pl.multiple_of(s * META, META), META), :128].astype(F32)
            cut = jnp.max(m[0:1, :] * 8.0 + m[1:2, :])
            other = jnp.max(m[2:3, :] * 8.0 + m[3:4, :])
            used = jnp.where(e == 0, cut, other).astype(jnp.int32)

            def tile_body(k, _):
                base = jnp.where(e == 0, k * TILE, PACK - TILE - k * TILE)
                r = pl.ds(pl.multiple_of(s * PACK + base, 64), TILE)
                row = (lax.broadcasted_iota(jnp.int32, (TILE, fs), 0) + base).astype(F32)
                keep = (cut - row - 0.5) * sign > 0.0
                h = jnp.dot(x[r, :], w13[e], preferred_element_type=F32).astype(BF16).astype(F32)
                da = lax.dot_general(y[r, :], w2s[e], (((1,), (1,)), ((), ())),
                                     preferred_element_type=F32).astype(BF16).astype(F32)
                h1 = jnp.where(keep, h[:, :fs], 0.0)
                h3 = jnp.where(keep, h[:, fs:], 0.0)
                da = jnp.where(keep, da, 0.0)
                sg = jax.nn.sigmoid(h1)
                silu = h1 * sg
                a[...] = (silu * h3).astype(BF16)
                dh[:, :fs] = (da * h3 * sg * (1.0 + h1 * (1.0 - sg))).astype(BF16)
                dh[:, fs:] = (da * silu).astype(BF16)
                for i in range(d // 256):
                    m = slice(i * 256, (i + 1) * 256)
                    acc13[e, m, :] += lax.dot_general(x[r, m], dh[...], (((0,), (0,)), ((), ())), preferred_element_type=F32)
                acc2[e] += lax.dot_general(a[...], y[r, :], (((0,), (0,)), ((), ())), preferred_element_type=F32)
                return 0

            lax.fori_loop(0, (used + (TILE - 1)) // TILE, tile_body, 0)
            return 0

        lax.fori_loop(0, n, group_body, 0)
        for c in out_copies(e):
            c.start()
        return 0

    lax.fori_loop(0, el, expert_body, 0)
    flag = ym[pl.ds(0, META), :].astype(F32)
    for s in range(1, n):
        flag = jnp.maximum(flag, ym[pl.ds(s * META, META), :].astype(F32))
    if not first:
        flag = jnp.maximum(flag, refs[4 * n + 6][...])
    oflag[...] = flag
    for e in range(el):
        for c in out_copies(e):
            c.wait()


def _dwp_call(idx, xs, ys, w1, w3, w2, prev):
    el, d, f = w1.shape
    n = len(xs)
    fs = f // 8
    anyspec = pl.BlockSpec(memory_space=pl.ANY)
    vspec = pl.BlockSpec(memory_space=pltpu.VMEM)
    outs = [jax.ShapeDtypeStruct((el, d, fs), F32), jax.ShapeDtypeStruct((el, d, fs), F32),
            jax.ShapeDtypeStruct((el, fs, d), F32), jax.ShapeDtypeStruct((META, d), F32)]
    args = [idx, *(c for p in xs for c in p), *(c for p in ys for c in p), w1, w3, w2]
    specs = [pl.BlockSpec(memory_space=pltpu.SMEM)] + [anyspec] * (len(args) - 1)
    alias = {}
    if prev is not None:
        alias = {len(args) + i: i for i in range(3)}
        args += list(prev)
        specs += [anyspec] * 3 + [vspec]
    return pl.pallas_call(
        functools.partial(_dwp_kernel, n, prev is None),
        out_shape=outs,
        in_specs=specs,
        out_specs=[anyspec] * 3 + [vspec],
        scratch_shapes=[
            pltpu.VMEM((n * PACK, d), BF16),
            pltpu.VMEM((n * PACK, d), BF16),
            pltpu.VMEM((n * META, d), BF16),
            pltpu.VMEM((n * META, d), BF16),
            pltpu.VMEM((el, d, 2 * fs), BF16),
            pltpu.VMEM((el, fs, d), BF16),
            pltpu.VMEM((TILE, 2 * fs), BF16),
            pltpu.VMEM((TILE, fs), BF16),
            pltpu.VMEM((el, d, 2 * fs), F32),
            pltpu.VMEM((el, fs, d), F32),
            pltpu.SemaphoreType.DMA((6, el)),
            pltpu.SemaphoreType.DMA((2, n)),
            pltpu.SemaphoreType.DMA((2, n)),
            pltpu.SemaphoreType.DMA((2, n)),
            pltpu.SemaphoreType.DMA((3, el)),
        ],
        input_output_aliases=alias,
        cost_estimate=pl.CostEstimate(flops=12 * n * PACK * d * fs, bytes_accessed=n * 4 * 2**20 + 18 * 2**20,
                                      transcendentals=n * PACK * fs),
    )(*args)


def _dw_kernel(e, n, first, idx_ref, *refs):
    xs, ys = refs[:n], refs[n:2 * n]
    w1, w3, w2 = refs[2 * n:2 * n + 3]
    o1, o3, o2 = refs[-15:-12]
    x, y, w13, w2s, dh, a, acc13, acc2, wsem, xsem, ysem, osem = refs[-12:]
    rows = xs[0].shape[0]
    fs = w2s.shape[0]
    tile = 64
    per = rows // tile
    f0 = pl.multiple_of(idx_ref[0] * fs, 128)
    half = lambda j: pl.ds(j * fs, fs)

    def row_copy(src, dst, j, sem):
        return pltpu.make_async_copy(src, dst.at[pl.ds(pl.multiple_of(j * rows, 64), rows)], sem.at[j])

    wcp = [
        pltpu.make_async_copy(w1.at[e, :, pl.ds(f0, fs)], w13.at[:, half(0)], wsem.at[0]),
        pltpu.make_async_copy(w3.at[e, :, pl.ds(f0, fs)], w13.at[:, half(1)], wsem.at[1]),
        pltpu.make_async_copy(w2.at[e, pl.ds(f0, fs), :], w2s, wsem.at[2]),
    ]
    row_copy(xs[0], x, 0, xsem).start()
    for c in wcp:
        c.start()
    row_copy(ys[0], y, 0, ysem).start()
    for j in range(1, n):
        row_copy(xs[j], x, j, xsem).start()
        row_copy(ys[j], y, j, ysem).start()
    prev = []
    if not first:
        prev = [
            pltpu.make_async_copy(o1.at[e], acc13.at[:, half(0)], wsem.at[3]),
            pltpu.make_async_copy(o3.at[e], acc13.at[:, half(1)], wsem.at[4]),
            pltpu.make_async_copy(o2.at[e], acc2, wsem.at[5]),
        ]
        for c in prev:
            c.start()
    for c in wcp:
        c.wait()

    def rows_body(i, _):
        @pl.when(lax.rem(i, per) == 0)
        def _():
            row_copy(xs[0], x, i // per, xsem).wait()
            row_copy(ys[0], y, i // per, ysem).wait()

        r = pl.ds(pl.multiple_of(i * tile, 64), tile)
        h = jnp.dot(x[r, :], w13[...], preferred_element_type=F32).astype(BF16).astype(F32)
        da = lax.dot_general(y[r, :], w2s[...], (((1,), (1,)), ((), ())),
                             preferred_element_type=F32).astype(BF16).astype(F32)
        h1, h3 = h[:, :fs], h[:, fs:]
        s = jax.nn.sigmoid(h1)
        silu = h1 * s
        a[r, :] = (silu * h3).astype(BF16)
        dh[r, :fs] = (da * h3 * s * (1.0 + h1 * (1.0 - s))).astype(BF16)
        dh[r, fs:] = (da * silu).astype(BF16)
        return 0

    lax.fori_loop(0, per * n, rows_body, 0)
    for c in prev:
        c.wait()

    def acc(ref, m, val):
        if first:
            ref[m, :] = val
        else:
            ref[m, :] += val

    def out_copies(i):
        m = pl.ds(pl.multiple_of(i * 256, 256), 256)
        return (pltpu.make_async_copy(acc13.at[m, half(0)], o1.at[e, m], osem.at[0]),
                pltpu.make_async_copy(acc13.at[m, half(1)], o3.at[e, m], osem.at[1]))

    def d13_body(i, _):
        m = pl.ds(pl.multiple_of(i * 256, 256), 256)
        acc(acc13, m, lax.dot_general(x[:, m], dh[...], (((0,), (0,)), ((), ())), preferred_element_type=F32))
        for c in out_copies(i):
            c.start()
        return 0

    nm = x.shape[1] // 256
    lax.fori_loop(0, nm, d13_body, 0)

    def d2_copy(i):
        m = pl.ds(pl.multiple_of(i * 128, 128), 128)
        return pltpu.make_async_copy(acc2.at[m], o2.at[e, m], osem.at[2])

    def d2_body(i, _):
        m = pl.ds(pl.multiple_of(i * 128, 128), 128)
        acc(acc2, m, lax.dot_general(a[:, m], y[...], (((0,), (0,)), ((), ())), preferred_element_type=F32))
        d2_copy(i).start()
        return 0

    lax.fori_loop(0, fs // 128, d2_body, 0)

    def drain13(i, _):
        for c in out_copies(i):
            c.wait()
        return 0

    def drain2(i, _):
        d2_copy(i).wait()
        return 0

    lax.fori_loop(0, nm, drain13, 0)
    lax.fori_loop(0, fs // 128, drain2, 0)


def _dw_call(e, idx, xs, ys, w1, w3, w2, prev, first):
    el, d, f = w1.shape
    n, rows = len(xs), xs[0].shape[0]
    fs = f // 8
    anyspec = pl.BlockSpec(memory_space=pl.ANY)
    outs = [jax.ShapeDtypeStruct((el, d, fs), F32), jax.ShapeDtypeStruct((el, d, fs), F32),
            jax.ShapeDtypeStruct((el, fs, d), F32)]
    args = [idx, *xs, *ys, w1, w3, w2]
    alias = {}
    if prev is not None:
        alias = {len(args) + i: i for i in range(3)}
        args += list(prev)
    return pl.pallas_call(
        functools.partial(_dw_kernel, e, n, first),
        out_shape=outs,
        in_specs=[pl.BlockSpec(memory_space=pltpu.SMEM)] + [anyspec] * (len(args) - 1),
        out_specs=[anyspec] * 3,
        scratch_shapes=[
            pltpu.VMEM((n * rows, d), BF16),
            pltpu.VMEM((n * rows, d), BF16),
            pltpu.VMEM((d, 2 * fs), BF16),
            pltpu.VMEM((fs, d), BF16),
            pltpu.VMEM((n * rows, 2 * fs), BF16),
            pltpu.VMEM((n * rows, fs), BF16),
            pltpu.VMEM((d, 2 * fs), F32),
            pltpu.VMEM((fs, d), F32),
            pltpu.SemaphoreType.DMA((6,)),
            pltpu.SemaphoreType.DMA((n,)),
            pltpu.SemaphoreType.DMA((n,)),
            pltpu.SemaphoreType.DMA((3,)),
        ],
        input_output_aliases=alias,
        cost_estimate=pl.CostEstimate(flops=12 * n * rows * d * fs, bytes_accessed=n * 2 * 2**20 + 9 * 2**20,
                                      transcendentals=n * rows * fs),
    )(*args)


def solution(mesh):
    np_ = mesh.shape['expert']
    tok = P(('data', 'expert'), None)
    buf = P(('data', 'expert'), None, None)
    wsp = P('expert', None, None)

    def body(dy, gates, topk_idx, slot, yd, xd, h1, h3, w1, w3, w2):
        d = dy.shape[1]
        el = w1.shape[0]
        cap = xd.shape[1] // np_
        idx = lax.axis_index('data').astype(jnp.int32).reshape(1)

        used = (jnp.max(jnp.abs(xd.astype(F32)), axis=-1) > 0.0).astype(BF16)
        rows = xd.shape[1]
        at = lax.broadcasted_iota(jnp.int32, (rows, rows), 0)
        to = lax.broadcasted_iota(jnp.int32, (rows, rows), 1)
        rank = jnp.dot(used, (at < to).astype(BF16), preferred_element_type=F32)
        count = jnp.sum(used.astype(F32), axis=1)
        room = PACK - count[0]
        far = jnp.where(rank[1] < room, PACK - 1 - rank[1], PACK + rank[1] - room)
        pos = jnp.where(used > 0, jnp.stack([rank[0], far]), -1.0).reshape(1, el * rows)
        kept = jnp.stack([count[0], jnp.minimum(count[1], room)])
        eighth = jnp.floor(kept / 8.0)
        meta = jnp.stack([eighth, kept - 8.0 * eighth], axis=1).reshape(4)
        over = (count[0] + count[1] > PACK).astype(F32)
        halves = ((0, FRONT, True), (FRONT, PACK - FRONT, False))

        def chain(c, last_right):
            r, l = [c], [c]
            for _ in range(3):
                r.append([lax.ppermute(v, 'data', RIGHT) for v in r[-1]])
                l.append([lax.ppermute(v, 'data', LEFT) for v in l[-1]])
            perm, last = (RIGHT, r[3]) if last_right else (LEFT, l[3])
            r.append([lax.ppermute(v, 'data', perm) for v in last])
            return r, l

        xr, xl = chain(_pack(xd, pos, meta, halves, el, False), True)

        v = (gates[:, :, None] * dy.astype(F32)[:, None, :]).astype(BF16)
        blk = el * cap + META
        ex, sl = topk_idx[:, 0], slot[:, 0]
        row = jnp.where(sl >= 0, ex * cap + (ex // el) * META + sl, -1).reshape(1, -1)
        send = _send(row, over.reshape(1), v[:, 0], np_, blk)
        recv = lax.all_to_all(send.reshape(np_, blk, d), 'expert', 0, 0, tiled=True)
        dyd = jnp.swapaxes(recv[:, :el * cap].reshape(np_, el, cap, d), 0, 1).reshape(el, np_ * cap, d)
        yr, yl = chain(_pack(recv, pos, meta, halves, el, True), False)
        dg = jnp.einsum('tkd,td->tk', yd, dy, preferred_element_type=F32)

        h1f = h1.astype(F32)
        h3f = h3.astype(F32)
        s = jax.nn.sigmoid(h1f)
        silu = h1f * s
        da = jnp.einsum('ecd,efd->ecf', dyd, w2, preferred_element_type=F32).astype(BF16).astype(F32)
        dh1 = (da * h3f * s * (1.0 + h1f * (1.0 - s))).astype(BF16)
        dh3 = (da * silu).astype(BF16)
        dxd = (jnp.einsum('ecf,edf->ecd', dh1, w1, preferred_element_type=F32)
               + jnp.einsum('ecf,edf->ecd', dh3, w3, preferred_element_type=F32)).astype(BF16)
        out = jnp.swapaxes(dxd.reshape(el, np_, cap, d), 0, 1)
        back = lax.all_to_all(out, 'expert', 0, 0, tiled=True).reshape(np_ * el * cap, d)
        dx = _unpack(jnp.where(sl >= 0, ex * cap + sl, -1)[:, None], back)

        acc = None
        for pick in (lambda r, l: (r[0], r[1], l[1]), lambda r, l: (r[2], l[2]),
                           lambda r, l: (r[3], l[3]), lambda r, l: (r[4],)):
            acc = _dwp_call(idx, pick(xr, xl), pick(yr, yl), w1, w3, w2, acc)

        acc, some = acc[:3], acc[3][0, 0] > 0
        rest = ((PACK, el * rows - PACK, False),)

        def spill(acc):
            xo, = _pack(xd, pos, meta, rest, el, False)
            yo, = _pack(recv, pos, meta, rest, el, True)

            acc = _dw_call(1, idx, [xo], [yo], w1, w3, w2, acc, False)

            def hop(_, st):
                xa, ya, xb, yb, acc = st
                xa, ya = (lax.ppermute(c, 'data', RIGHT) for c in (xa, ya))
                xb, yb = (lax.ppermute(c, 'data', LEFT) for c in (xb, yb))
                return xa, ya, xb, yb, tuple(_dw_call(1, idx, [xa, xb], [ya, yb], w1, w3, w2, acc, False))

            xa, ya, _, _, acc = lax.fori_loop(0, 3, hop, (xo, yo, xo, yo, tuple(acc)))
            xa, ya = (lax.ppermute(c, 'data', RIGHT) for c in (xa, ya))
            return tuple(_dw_call(1, idx, [xa], [ya], w1, w3, w2, acc, False))

        acc = lax.cond(some, spill, lambda acc: acc, tuple(acc))
        dw1, dw3, dw2 = acc
        return dx, dg, dw1, dw3, dw2

    return jax.shard_map(body, mesh=mesh,
                         in_specs=(tok, tok, tok, tok, buf, buf, buf, buf, wsp, wsp, wsp),
                         out_specs=(tok, tok, P('expert', None, 'data'), P('expert', None, 'data'), P('expert', 'data', None)),
                         check_vma=False)
```
